128 devices in a mesh: rows: 16 (over x, z), cols: 8 (over y, core).
Axes of the slice: x: 4, y: 4, z: 4, core: 2. Of those that a mesh axis runs over, the one named last changes fastest.
Arguments:
- margins: bfloat16 [16384, 2048], P(('rows', 'cols')), may hold values from -512 to 512
- subset_masks: bfloat16 [16384, 8192], P('rows'), may hold values from 0 to 1
- ridge_param: float32 [], replicated, may hold values from 2048 to 8192
Outputs:
- weights: float32 [8192, 2048], P('rows', 'cols')
- residual_norm: float32 [2048], P('cols')
The draws below stay inside these ranges and needn't reach their ends.
All inputs are finite; a program needn't handle non-finite values.
Results may differ from the reference program's by a relative error of at most 0.0021.
Values may be sent and summed in bfloat16 or wider, within the bound.
A program may use at most 128 MiB of HBM per device.

```python
import math
import jax
import jax.numpy as jnp
from jax import lax

N = 8192
E = 2048
ITERS = 2
M = 16384


def draw_subset_masks(key, part):
    uniform = jax.random.uniform(key, (M, N), jnp.float32)
    return (uniform < 0.5).astype(jnp.float32).astype(jnp.bfloat16)


def block_scale(rng, extent, pieces, smallest, high):
    level, own = 1.0, jax.random.fold_in(rng, 6)
    for position, shards_of in pieces:
        steps = jnp.exp(jax.random.uniform(jax.random.fold_in(own, position), (shards_of,), jnp.float32, smallest / len(pieces), high / len(pieces)))
        level = level * jnp.repeat(steps, extent[position] // shards_of).reshape([-1 if axis == position else 1 for axis in range(len(extent))])
    return level


def normal_values(key, dims, deviation, reach, split=(), dtype=jnp.bfloat16):
    result = jax.random.normal(key, dims, jnp.float32) * deviation
    if len(split) > 0:
        result = block_scale(key, dims, split, -0.22, 0.18) * result
    return jnp.clip(result, min=-reach, max=reach).astype(dtype)


def setup_inputs(seed: int = 0) -> dict:
    arg_keys = jax.random.split(jax.random.key(seed), 4)
    margins = normal_values(arg_keys[0], (M, E), 64.0, 512.0, ((0, 128),))
    subset_masks = draw_subset_masks(jax.random.fold_in(arg_keys[3], 71), 0)
    ridge_param = jnp.clip(jnp.exp(jax.random.uniform(arg_keys[2], (), jnp.float32, math.log(2048.0), math.log(8192.0))), 2048.0, 8192.0)
    return dict(margins=margins, subset_masks=subset_masks, ridge_param=ridge_param)


def rounded(values):
    low = lax.optimization_barrier(values.astype(jnp.bfloat16))
    return low.astype(jnp.float32)

def reference(margins, subset_masks, ridge_param):
    design = 2.0 * subset_masks.astype(jnp.float32) - 1.0
    highest = lax.Precision.HIGHEST
    target = jnp.dot(design.T, margins.astype(jnp.float32), precision=highest)
    first_norms = lax.optimization_barrier(jnp.sum(target * target, axis=0))
    weights = jnp.zeros_like(target)
    residual = target
    direction = target
    norm_now = first_norms
    for iteration in range(ITERS):
        dir_low = rounded(direction)
        fitted = jnp.dot(design, dir_low, precision=highest)
        fitted_low = rounded(fitted)
        image = jnp.dot(design.T, fitted_low, precision=highest) + ridge_param * direction
        curvature = lax.optimization_barrier(jnp.sum(dir_low * image, axis=0))
        alpha = norm_now / curvature
        weights = weights + alpha * direction
        residual = residual - alpha * image
        norm_next = lax.optimization_barrier(jnp.sum(residual * residual, axis=0))
        direction = residual + norm_next / norm_now * direction
        norm_now = norm_next
    return (weights, jnp.sqrt(norm_now / first_norms))
```

```python
import functools

import jax
import jax.numpy as jnp
from jax import lax
from jax.experimental import pallas as pl
from jax.experimental.pallas import tpu as pltpu
from jax.sharding import PartitionSpec as P

MESH = pl.DeviceIdType.MESH
BF16 = jnp.bfloat16
F32 = jnp.float32
SIDE = 4
LOADS = 8

FIRST_SLOT = ({2: 4, 0: 5, 1: 2, 3: 3}, {2: 2, 0: 3, 1: 4, 3: 5})
GATHER_ORDER = ((0, 1, 3, 2), (0, 3, 1, 2))
GATHER_PASS = ((0, 3), (1, 2))


def fit(
    cols_size, ridge_ref, margins_ref, mask_ref, w_ref, rn_ref,
    design, regrouped, dir_all, image_all, fit_one, fit_two, fit_low, own, target, image,
    wide_s1, wide_r1, wide_s2, wide_r2, low_s1, low_r1, low_s2, low_r2, ex_s, ex_r,
    load_sem, m_send, m_recv, s1_send, s1_recv, s2_send, s2_recv,
    a1_send, a1_recv, a2_send, a2_recv, ex_send, ex_recv,
):
    row = lax.axis_index("rows")
    col = lax.axis_index("cols")
    x, z = lax.div(row, SIDE), lax.rem(row, SIDE)
    depth, examples = design.shape
    block = examples // (SIDE * SIDE)
    half = block // 2
    quarter = half // 2
    evals = target.shape[1]
    per = depth // cols_size
    ridge = ridge_ref[0, 0]

    def row_of(h, u1, u2):
        return lax.rem(u1 + 8, SIDE) * (4 - 3 * h) + lax.rem(u2 + 8, SIDE) * (1 + 3 * h)

    def c1(h):
        return x * (1 - h) + z * h

    def c2(h):
        return z * (1 - h) + x * h

    def first(h, u1, u2):
        return pl.multiple_of(row_of(h, u1, u2) * block + h * half, half)

    def load(i):
        rows = pl.ds(i * (depth // LOADS), depth // LOADS)
        return pltpu.make_async_copy(mask_ref.at[rows], design.at[rows], load_sem.at[i])

    def line(i):
        return lax.rem(x + i, SIDE) * SIDE + z, x * SIDE + lax.rem(z + i, SIDE)

    for i in range(LOADS):
        load(i).start()

    barrier = pltpu.get_barrier_semaphore()
    for i in range(1, SIDE):
        for peer in line(i):
            pl.semaphore_signal(barrier, inc=1, device_id={"rows": peer}, device_id_type=MESH)
    for i in range(1, cols_size):
        peer = lax.rem(col + i, cols_size)
        pl.semaphore_signal(barrier, inc=1, device_id={"cols": peer}, device_id_type=MESH)
    pl.semaphore_wait(barrier, 2 * (SIDE - 1) + cols_size - 1)

    def hand_over(i):
        peer = lax.rem(col + i, cols_size)
        return pltpu.make_async_remote_copy(
            margins_ref.at[:, pl.ds(pl.multiple_of(peer * evals, evals), evals)],
            regrouped.at[pl.ds(pl.multiple_of(col * per, per), per)],
            m_send.at[i - 1],
            m_recv.at[i - 1],
            device_id={"cols": peer},
            device_id_type=MESH,
        )

    for i in range(1, cols_size):
        hand_over(i).start()
    regrouped[pl.ds(pl.multiple_of(col * per, per), per)] = margins_ref[
        :, pl.ds(pl.multiple_of(col * evals, evals), evals)
    ]

    step = min(16, depth // LOADS)
    for i in range(LOADS):
        load(i).wait()

        @pl.loop(0, depth // LOADS // step)
        def _(j):
            rows = pl.ds(pl.multiple_of(i * (depth // LOADS) + j * step, step), step)
            design[rows] = design[rows] * 2 - 1

    for i in range(1, cols_size):
        hand_over(i).wait()

    def partial(operand, h, u1, u2):
        return lax.dot_general(
            design[:, pl.ds(first(h, u1, u2), half)],
            operand[...],
            (((0,), (0,)), ((), ())),
            preferred_element_type=F32,
        )

    def reduce_scatter(operand, s1, r1, s2, r2, after_far, after_own, done):
        kind = s1.dtype

        def send1(h, d, slot):
            return pltpu.make_async_remote_copy(
                s1.at[h, d, slot],
                r1.at[h, d, slot],
                s1_send.at[h, d, slot],
                s1_recv.at[h, d, slot],
                device_id={"rows": row_of(h, c1(h) + 1 - 2 * d, c2(h))},
                device_id_type=MESH,
            )

        def send2(h, d, slot):
            return pltpu.make_async_remote_copy(
                s2.at[h, d, slot],
                r2.at[h, d, slot],
                s2_send.at[h, d, slot],
                s2_recv.at[h, d, slot],
                device_id={"rows": row_of(h, c1(h), c2(h) + 1 - 2 * d)},
                device_id_type=MESH,
            )

        def parts(i):
            return lax.rem(i, 2), lax.rem(lax.div(i, 2), 2), lax.div(i, 4)

        @pl.loop(0, 8)
        def _(i):
            h, d, s = parts(i)
            k = (2 - d) * (1 - s) + 3 * d * s
            s1[h, d, s] = partial(operand, h, c1(h) + 2, c2(h) + k).astype(kind)
            send1(h, d, s).start()

        @pl.loop(0, 8)
        def _(i):
            h, d, s = parts(i)
            k = (1 + d) * (1 - s) + 3 * (1 - d) * s
            s1[h, d, 2 + s] = partial(operand, h, c1(h) + 1 - 2 * d, c2(h) + k).astype(kind)
            send1(h, d, 2 + s).start()

        after_far()

        @pl.loop(0, 8)
        def _(i):
            h, d, s = parts(i)
            k = (2 - d) * (1 - s) + 3 * d * s
            here = partial(operand, h, c1(h) + 1 - 2 * d, c2(h) + k)
            send1(h, d, s).wait_recv()
            s1[h, d, 4 + s] = (here + r1[h, d, s].astype(F32)).astype(kind)
            send1(h, d, 4 + s).start()

        @pl.loop(0, 8)
        def _(i):
            h, k = lax.rem(i, 2), lax.div(i, 2)
            own[h, k] = partial(operand, h, c1(h), c2(h) + k)

        after_own()

        def collect(h, k):
            for d in (0, 1):
                send1(h, d, FIRST_SLOT[d][k]).wait_recv()
            own[h, k] = (
                own[h, k]
                + r1[h, 0, FIRST_SLOT[0][k]].astype(F32)
                + r1[h, 1, FIRST_SLOT[1][k]].astype(F32)
            )

        def part(h, k, j):
            return own[h, k, pl.ds(j * quarter, quarter)]

        for h in (0, 1):
            collect(h, 2)
            for d in (0, 1):
                s2[h, d, 0] = part(h, 2, d).astype(kind)
                send2(h, d, 0).start()
        for d, k in ((0, 1), (1, 3)):
            for h in (0, 1):
                collect(h, k)
                s2[h, d, 1] = part(h, k, 1 - d).astype(kind)
                send2(h, d, 1).start()
        for h in (0, 1):
            for d, k in ((0, 1), (1, 3)):
                send2(h, d, 0).wait_recv()
                s2[h, d, 2] = (part(h, k, d) + r2[h, d, 0].astype(F32)).astype(kind)
                send2(h, d, 2).start()
        for h in (0, 1):
            collect(h, 0)
        for h in (0, 1):
            sums = []
            for j in (0, 1):
                send2(h, j, 2).wait_recv()
                send2(h, 1 - j, 1).wait_recv()
                sums.append(
                    part(h, 0, j) + r2[h, j, 2].astype(F32) + r2[h, 1 - j, 1].astype(F32)
                )
            done(h, sums)

        def drain():
            @pl.loop(0, 24)
            def _(i):
                send1(lax.rem(i, 2), lax.rem(lax.div(i, 2), 2), lax.div(i, 4)).wait_send()

            @pl.loop(0, 12)
            def _(i):
                send2(lax.rem(i, 2), lax.rem(lax.div(i, 2), 2), lax.div(i, 4)).wait_send()

        return drain

    def gather_steps(everything):
        def copy(rows, sends, recvs, h, d, slot, peer):
            return pltpu.make_async_remote_copy(
                everything.at[rows],
                everything.at[rows],
                sends.at[h, d, slot],
                recvs.at[h, d, slot],
                device_id={"rows": peer},
                device_id_type=MESH,
            )

        def send1(h, d, slot):
            sign = 1 - 2 * d
            if slot == 0:
                rows = pl.ds(first(h, c1(h), c2(h)), half)
            else:
                start = first(h, c1(h), c2(h) - sign) + d * quarter
                rows = pl.ds(pl.multiple_of(start, quarter), quarter)
            return copy(rows, a1_send, a1_recv, h, d, slot, row_of(h, c1(h), c2(h) + sign))

        def send2(h, d, slot):
            sign = 1 - 2 * d
            if slot < 4:
                rows = pl.ds(first(h, c1(h), c2(h) + GATHER_ORDER[d][slot]), half)
            else:
                rows = pl.ds(first(h, c1(h) - sign, c2(h) + GATHER_PASS[d][slot - 4]), half)
            return copy(rows, a2_send, a2_recv, h, d, slot, row_of(h, c1(h) + sign, c2(h)))

        return send1, send2

    def gather_start(everything, h):
        send1, send2 = gather_steps(everything)
        for d in (0, 1):
            send1(h, d, 0).start()
        for d in (0, 1):
            send2(h, d, 0).start()

    def gather_and_multiply(everything, result, meanwhile):
        send1, send2 = gather_steps(everything)
        tile = min(256, depth)

        def multiply(places, fresh=False):
            starts = [first(h, c1(h) + u1, c2(h) + u2) for h in (0, 1) for u1, u2 in places]

            @pl.loop(0, depth // tile)
            def _(i):
                rows = pl.ds(pl.multiple_of(i * tile, tile), tile)
                total = None
                for start in starts:
                    term = jnp.dot(
                        design[rows, pl.ds(start, half)],
                        everything[pl.ds(start, half)],
                        preferred_element_type=F32,
                    )
                    total = term if total is None else total + term
                result[rows] = total if fresh else result[rows] + total

        multiply([(0, 0)], fresh=True)
        for h in (0, 1):
            for d in (0, 1):
                send1(h, d, 0).wait_recv()
                send1(h, d, 1).start()
        for h in (0, 1):
            for slot in (1, 2):
                for d in (0, 1):
                    send2(h, d, slot).start()
        meanwhile[0]()
        multiply([(0, 1), (0, 3)])
        for h in (0, 1):
            for d in (0, 1):
                send1(h, d, 1).wait_recv()
            for d in (0, 1):
                send2(h, d, 3).start()
        multiply([(0, 2)])
        meanwhile[1]()
        for h in (0, 1):
            for d in (0, 1):
                send2(h, d, 0).wait_recv()
            send2(h, 0, 4).start()
        multiply([(-1, 0), (1, 0)])
        for h in (0, 1):
            for slot in (1, 2):
                for d in (0, 1):
                    send2(h, d, slot).wait_recv()
            send2(h, 0, 5).start()
            send2(h, 1, 4).start()
        multiply([(-1, 1), (1, 3)])
        multiply([(-1, 3), (1, 1)])
        for h in (0, 1):
            for d in (0, 1):
                send2(h, d, 3).wait_recv()
            send2(h, 1, 5).start()
        multiply([(-1, 2), (1, 2)])
        meanwhile[2]()
        for slot in (4, 5):
            for h in (0, 1):
                for d in (0, 1):
                    send2(h, d, slot).wait_recv()
            multiply([(2, GATHER_PASS[0][slot - 4]), (2, GATHER_PASS[1][slot - 4])])
        for h in (0, 1):
            for d in (0, 1):
                for slot in range(2):
                    send1(h, d, slot).wait_send()
                for slot in range(6):
                    send2(h, d, slot).wait_send()

    def exchange(e, stage, i):
        return pltpu.make_async_remote_copy(
            ex_s.at[e, stage],
            ex_r.at[e, stage, i - 1],
            ex_send.at[e, stage, i - 1],
            ex_recv.at[e, stage, i - 1],
            device_id={"rows": line(i)[stage]},
            device_id_type=MESH,
        )

    def exchange_start(e, stage):
        for i in range(1, SIDE):
            exchange(e, stage, i).start()

    def exchange_sum(e, stage):
        total = ex_s[e, stage]
        for i in range(1, SIDE):
            exchange(e, stage, i).wait()
            total = total + ex_r[e, stage, i - 1]
        return total

    def exchange_turn(e):
        ex_s[e, 1] = exchange_sum(e, 0)
        exchange_start(e, 1)

    def total(values):
        return jnp.sum(values, axis=0, keepdims=True)

    def low(values):
        return values.astype(BF16).astype(F32)

    def nothing():
        pass

    def keep(store, everything):
        def done(h, sums):
            for j in (0, 1):
                rows = pl.ds(h * half + j * quarter, quarter)
                store[rows] = sums[j]
                at = pl.multiple_of(row * block + h * half + j * quarter, quarter)
                everything[pl.ds(at, quarter)] = sums[j].astype(BF16)
            gather_start(everything, h)

        return done

    drain = reduce_scatter(
        regrouped, wide_s1, wide_r1, wide_s2, wide_r2, nothing, nothing, keep(target, dir_all)
    )
    gather_and_multiply(dir_all, fit_one, (nothing, drain, nothing))

    fit_low[...] = fit_one[...].astype(BF16)

    ex_s[0, 0] = jnp.zeros_like(ex_s[0, 0])
    ex_s[0, 0, pl.ds(0, 1)] = total(target[...] * target[...])
    ex_s[0, 0, pl.ds(1, 1)] = total(fit_one[...] * fit_low[...].astype(F32)) + ridge * total(
        low(target[...]) * target[...]
    )
    exchange_start(0, 0)

    drain = reduce_scatter(
        fit_low, low_s1, low_r1, low_s2, low_r2,
        functools.partial(exchange_turn, 0), nothing, keep(image, image_all),
    )
    sums = exchange_sum(0, 1)
    first_norms = sums[0:1]
    alpha_one = first_norms / sums[1:2]

    def residual_one():
        return target[...] - alpha_one * (image[...] + ridge * target[...])

    ex_s[1, 0] = jnp.zeros_like(ex_s[1, 0])
    ex_s[1, 0, pl.ds(0, 1)] = total(residual_one() * residual_one())
    exchange_start(1, 0)

    def middle():
        exchange_turn(1)
        drain()

    gather_and_multiply(image_all, fit_two, (nothing, middle, nothing))
    norm_one = exchange_sum(1, 1)[0:1]
    beta = norm_one / first_norms
    fit_two[...] = (1 + beta - alpha_one * ridge) * fit_one[...] - alpha_one * fit_two[...]
    fit_low[...] = fit_two[...].astype(BF16)

    ex_s[2, 0] = jnp.zeros_like(ex_s[2, 0])
    residual = residual_one()
    direction = residual + beta * target[...]
    w_ref[...] = alpha_one * target[...]
    image[...] = residual
    target[...] = direction
    ex_s[2, 0, pl.ds(0, 1)] = total(fit_two[...] * fit_low[...].astype(F32)) + ridge * total(
        low(target[...]) * target[...]
    )
    exchange_start(2, 0)

    def second_weights():
        alpha_two = norm_one / exchange_sum(2, 1)[0:1]
        ex_s[3, 1, pl.ds(0, 1)] = alpha_two
        w_ref[...] = w_ref[...] + alpha_two * target[...]

    def residual_two(h, sums):
        alpha_two = ex_s[3, 1, pl.ds(0, 1)]
        squares = None
        for j in (0, 1):
            rows = pl.ds(h * half + j * quarter, quarter)
            left = image[rows] - alpha_two * (sums[j] + ridge * target[rows])
            square = total(left * left)
            squares = square if squares is None else squares + square
        ex_s[3, 0, pl.ds(h, 1)] = squares

    ex_s[3, 0] = jnp.zeros_like(ex_s[3, 0])
    drain = reduce_scatter(
        fit_low, low_s1, low_r1, low_s2, low_r2,
        functools.partial(exchange_turn, 2), second_weights, residual_two,
    )
    exchange_start(3, 0)
    exchange_turn(3)
    drain()
    squares = exchange_sum(3, 1)
    rn_ref[...] = jnp.sqrt((squares[0:1] + squares[1:2]) / first_norms)


def per_device(cols_size, margins, subset_masks, ridge_param):
    depth, examples = subset_masks.shape
    evals = margins.shape[1] // cols_size
    block = examples // (SIDE * SIDE)
    half, quarter = block // 2, block // 4
    vmem = pl.BlockSpec(memory_space=pltpu.VMEM)
    first = (2, 2, 6, half, evals)
    second = (2, 2, 3, quarter, evals)
    weights, norms = pl.pallas_call(
        functools.partial(fit, cols_size),
        out_shape=(
            jax.ShapeDtypeStruct((block, evals), F32),
            jax.ShapeDtypeStruct((1, evals), F32),
        ),
        in_specs=[
            pl.BlockSpec(memory_space=pltpu.SMEM),
            vmem,
            pl.BlockSpec(memory_space=pl.ANY),
        ],
        out_specs=(vmem, vmem),
        scratch_shapes=[
            pltpu.VMEM((depth, examples), BF16),
            pltpu.VMEM((depth, evals), BF16),
            pltpu.VMEM((examples, evals), BF16),
            pltpu.VMEM((examples, evals), BF16),
            pltpu.VMEM((depth, evals), F32),
            pltpu.VMEM((depth, evals), F32),
            pltpu.VMEM((depth, evals), BF16),
            pltpu.VMEM((2, SIDE, half, evals), F32),
            pltpu.VMEM((block, evals), F32),
            pltpu.VMEM((block, evals), F32),
            pltpu.VMEM(first, F32),
            pltpu.VMEM(first, F32),
            pltpu.VMEM(second, F32),
            pltpu.VMEM(second, F32),
            pltpu.VMEM(first, BF16),
            pltpu.VMEM(first, BF16),
            pltpu.VMEM(second, BF16),
            pltpu.VMEM(second, BF16),
            pltpu.VMEM((4, 2, 8, evals), F32),
            pltpu.VMEM((4, 2, SIDE - 1, 8, evals), F32),
            pltpu.SemaphoreType.DMA((LOADS,)),
            pltpu.SemaphoreType.DMA((max(cols_size - 1, 1),)),
            pltpu.SemaphoreType.DMA((max(cols_size - 1, 1),)),
            pltpu.SemaphoreType.DMA((2, 2, 6)),
            pltpu.SemaphoreType.DMA((2, 2, 6)),
            pltpu.SemaphoreType.DMA((2, 2, 3)),
            pltpu.SemaphoreType.DMA((2, 2, 3)),
            pltpu.SemaphoreType.DMA((2, 2, 2)),
            pltpu.SemaphoreType.DMA((2, 2, 2)),
            pltpu.SemaphoreType.DMA((2, 2, 6)),
            pltpu.SemaphoreType.DMA((2, 2, 6)),
            pltpu.SemaphoreType.DMA((4, 2, SIDE - 1)),
            pltpu.SemaphoreType.DMA((4, 2, SIDE - 1)),
        ],
        compiler_params=pltpu.CompilerParams(
            collective_id=0, has_side_effects=True, vmem_limit_bytes=66_000_000
        ),
    )(ridge_param.reshape(1, 1), margins, subset_masks)
    return weights, norms.reshape(evals)


def solution(mesh):
    in_specs = (P(("rows", "cols"), None), P("rows", None), P())
    out_specs = (P("rows", "cols"), P("cols"))
    return jax.shard_map(
        functools.partial(per_device, mesh.shape["cols"]),
        mesh=mesh, in_specs=in_specs, out_specs=out_specs, check_vma=False,
    )
```

```python
import functools

import jax
import jax.numpy as jnp
from jax import lax
from jax.experimental import pallas as pl
from jax.experimental.pallas import tpu as pltpu
from jax.sharding import PartitionSpec as P

MESH = pl.DeviceIdType.MESH
BF16 = jnp.bfloat16
F32 = jnp.float32
SIDE = 4
LOADS = 8

FIRST_SLOT = ({2: 2, 1: 1, 3: 4, 0: 5}, {2: 0, 1: 3, 3: 4, 0: 5})
SPAN = 2.0**15.75
GATHER_ORDER = ((0, 1, 3, 2), (0, 3, 1, 2))
GATHER_PASS = ((0, 3), (1, 2))


def fit(
    cols_size, ridge_ref, margins_hbm, mask_ref, w_ref, rn_ref,
    design, regrouped, dir_all, image_all, fit_one, fit_two, fit_low, own, target, image,
    s1, r1, s2, r2, ex_s, ex_r, margins,
    load_sem, margins_sem, m_send, m_recv, s1_send, s1_recv, s2_send, s2_recv,
    a1_send, a1_recv, a2_send, a2_recv, ex_send, ex_recv,
):
    row = lax.axis_index("rows")
    col = lax.axis_index("cols")
    x, z = lax.div(row, SIDE), lax.rem(row, SIDE)
    depth, examples = design.shape
    block = examples // (SIDE * SIDE)
    half = block // 2
    quarter = half // 2
    evals = target.shape[1]
    per = depth // cols_size
    ridge = ridge_ref[0, 0]

    def row_of(h, u1, u2):
        return lax.rem(u1 + 8, SIDE) * (4 - 3 * h) + lax.rem(u2 + 8, SIDE) * (1 + 3 * h)

    def c1(h):
        return x * (1 - h) + z * h

    def c2(h):
        return z * (1 - h) + x * h

    def first(h, u1, u2):
        return pl.multiple_of(row_of(h, u1, u2) * block + h * half, half)

    def load(i):
        rows = pl.ds(i * (depth // LOADS), depth // LOADS)
        return pltpu.make_async_copy(mask_ref.at[rows], design.at[rows], load_sem.at[i])

    def line(i):
        return lax.rem(x + i, SIDE) * SIDE + z, x * SIDE + lax.rem(z + i, SIDE)

    margins_load = pltpu.make_async_copy(margins_hbm, margins, margins_sem)
    margins_load.start()
    for i in range(LOADS):
        load(i).start()

    barrier = pltpu.get_barrier_semaphore()
    for i in range(1, SIDE):
        for peer in line(i):
            pl.semaphore_signal(barrier, inc=1, device_id={"rows": peer}, device_id_type=MESH)
    for i in range(1, cols_size):
        peer = lax.rem(col + i, cols_size)
        pl.semaphore_signal(barrier, inc=1, device_id={"cols": peer}, device_id_type=MESH)
    pl.semaphore_wait(barrier, 2 * (SIDE - 1) + cols_size - 1)

    def hand_over(i):
        peer = lax.rem(col + i, cols_size)
        return pltpu.make_async_remote_copy(
            margins.at[:, pl.ds(pl.multiple_of(peer * evals, evals), evals)],
            regrouped.at[pl.ds(pl.multiple_of(col * per, per), per)],
            m_send.at[i - 1],
            m_recv.at[i - 1],
            device_id={"cols": peer},
            device_id_type=MESH,
        )

    margins_load.wait()
    for i in range(1, cols_size):
        hand_over(i).start()
    regrouped[pl.ds(pl.multiple_of(col * per, per), per)] = margins[
        :, pl.ds(pl.multiple_of(col * evals, evals), evals)
    ]

    step = min(16, depth // LOADS)
    for i in range(LOADS):
        load(i).wait()

        @pl.loop(0, depth // LOADS // step)
        def _(j):
            rows = pl.ds(pl.multiple_of(i * (depth // LOADS) + j * step, step), step)
            design[rows] = design[rows] * 2 - 1

    for i in range(1, cols_size):
        hand_over(i).wait()

    def partial(operand, h, u1, u2):
        return lax.dot_general(
            design[:, pl.ds(first(h, u1, u2), half)],
            operand[...],
            (((0,), (0,)), ((), ())),
            preferred_element_type=F32,
        )

    def reduce_scatter(operand, encode, decode, after_far, after_own, done):
        def send1(h, d, slot):
            return pltpu.make_async_remote_copy(
                s1.at[h, d, slot],
                r1.at[h, d, slot],
                s1_send.at[h, d, slot],
                s1_recv.at[h, d, slot],
                device_id={"rows": row_of(h, c1(h) + 1 - 2 * d, c2(h))},
                device_id_type=MESH,
            )

        def send2(h, d, slot):
            return pltpu.make_async_remote_copy(
                s2.at[h, d, slot],
                r2.at[h, d, slot],
                s2_send.at[h, d, slot],
                s2_recv.at[h, d, slot],
                device_id={"rows": row_of(h, c1(h), c2(h) + 1 - 2 * d)},
                device_id_type=MESH,
            )

        def parts(i):
            return lax.rem(i, 2), lax.rem(lax.div(i, 2), 2), lax.div(i, 4)

        def send_block(h, d, slot, far, k, add, source):
            target = c1(h) + 2 * far + (1 - far) * (1 - 2 * d)
            here = partial(operand, h, target, c2(h) + k)

            if add is None:
                s1[h, d, slot] = encode(here, 1, h, d, 0)
            else:

                @pl.when(add == 1)
                def _():
                    send1(h, d, source).wait_recv()
                    there = decode(r1[h, d, source], 1, h, d, 0)
                    s1[h, d, slot] = encode(here + there, 1, h, d, 1)

                @pl.when(add == 0)
                def _():
                    s1[h, d, slot] = encode(here, 1, h, d, 0)

            send1(h, d, slot).start()

        @pl.loop(0, 8)
        def _(i):
            h, d, s = parts(i)
            send_block(h, d, s, 1 - (s - d) * (s - d), 2 - s, None, None)

        @pl.loop(0, 8)
        def _(i):
            h, k = lax.rem(i, 2), lax.div(i, 2)
            own[h, k] = partial(operand, h, c1(h), c2(h) + k)

        after_far()

        @pl.loop(0, 8)
        def _(i):
            h, d, s = parts(i)
            add = 1 - (s - d) * (s - d)
            send_block(h, d, 2 + s, 1 - add, d + 2 * (1 - s), add, d)

        after_own()

        def collect(h, k):
            for d in (0, 1):
                slot = FIRST_SLOT[d][k]
                summed = int((d, slot) in ((0, 2), (0, 5), (1, 3), (1, 4)))
                send1(h, d, slot).wait_recv()
                own[h, k] = own[h, k] + decode(r1[h, d, slot], 1, h, d, summed)

        def part(h, k, j):
            return own[h, k, pl.ds(j * quarter, quarter)]

        for h in (0, 1):
            collect(h, 2)
            for d in (0, 1):
                s2[h, d, 0] = encode(part(h, 2, d), 2, h, d, 0)
                send2(h, d, 0).start()

        @pl.loop(0, 8)
        def _(i):
            h, d, s = parts(i)
            add = s + d - 2 * s * d
            send_block(h, d, 4 + s, s * 0, 3 * (1 - s), add, 3 - d)

        for d, k in ((0, 1), (1, 3)):
            for h in (0, 1):
                collect(h, k)
                s2[h, d, 1] = encode(part(h, k, 1 - d), 2, h, d, 0)
                send2(h, d, 1).start()
        for d, k in ((0, 1), (1, 3)):
            for h in (0, 1):
                send2(h, d, 0).wait_recv()
                there = decode(r2[h, d, 0], 2, h, d, 0)
                s2[h, d, 2] = encode(part(h, k, d) + there, 2, h, d, 1)
                send2(h, d, 2).start()
        for h in (0, 1):
            collect(h, 0)
        for h in (0, 1):
            sums = []
            for j in (0, 1):
                send2(h, j, 2).wait_recv()
                send2(h, 1 - j, 1).wait_recv()
                sums.append(
                    part(h, 0, j)
                    + decode(r2[h, j, 2], 2, h, j, 1)
                    + decode(r2[h, 1 - j, 1], 2, h, 1 - j, 0)
                )
            done(h, sums)

        def drain():
            @pl.loop(0, 24)
            def _(i):
                send1(lax.rem(i, 2), lax.rem(lax.div(i, 2), 2), lax.div(i, 4)).wait_send()

            @pl.loop(0, 12)
            def _(i):
                send2(lax.rem(i, 2), lax.rem(lax.div(i, 2), 2), lax.div(i, 4)).wait_send()

        return drain

    def gather_steps(everything):
        def copy(rows, sends, recvs, h, d, slot, peer):
            return pltpu.make_async_remote_copy(
                everything.at[rows],
                everything.at[rows],
                sends.at[h, d, slot],
                recvs.at[h, d, slot],
                device_id={"rows": peer},
                device_id_type=MESH,
            )

        def send1(h, d, slot):
            sign = 1 - 2 * d
            if slot == 0:
                rows = pl.ds(first(h, c1(h), c2(h)), half)
            else:
                start = first(h, c1(h), c2(h) - sign) + d * quarter
                rows = pl.ds(pl.multiple_of(start, quarter), quarter)
            return copy(rows, a1_send, a1_recv, h, d, slot, row_of(h, c1(h), c2(h) + sign))

        def send2(h, d, slot):
            sign = 1 - 2 * d
            if slot < 4:
                rows = pl.ds(first(h, c1(h), c2(h) + GATHER_ORDER[d][slot]), half)
            else:
                rows = pl.ds(first(h, c1(h) - sign, c2(h) + GATHER_PASS[d][slot - 4]), half)
            return copy(rows, a2_send, a2_recv, h, d, slot, row_of(h, c1(h) + sign, c2(h)))

        return send1, send2

    def gather_start(everything, h):
        send1, send2 = gather_steps(everything)
        for d in (0, 1):
            send1(h, d, 0).start()
        for d in (0, 1):
            send2(h, d, 0).start()

    def gather_and_multiply(everything, result, meanwhile):
        send1, send2 = gather_steps(everything)
        tile = depth

        def multiply(places, fresh=False):
            starts = [first(h, c1(h) + u1, c2(h) + u2) for h in (0, 1) for u1, u2 in places]

            @pl.loop(0, depth // tile)
            def _(i):
                rows = pl.ds(pl.multiple_of(i * tile, tile), tile)
                total = None
                for start in starts:
                    term = jnp.dot(
                        design[rows, pl.ds(start, half)],
                        everything[pl.ds(start, half)],
                        preferred_element_type=F32,
                    )
                    total = term if total is None else total + term
                result[rows] = total if fresh else result[rows] + total

        multiply([(0, 0)], fresh=True)
        for h in (0, 1):
            for d in (0, 1):
                send1(h, d, 0).wait_recv()
                send1(h, d, 1).start()
        for h in (0, 1):
            for slot in (1, 2):
                for d in (0, 1):
                    send2(h, d, slot).start()
        meanwhile[0]()
        multiply([(0, 1), (0, 3)])
        for h in (0, 1):
            for d in (0, 1):
                send1(h, d, 1).wait_recv()
            for d in (0, 1):
                send2(h, d, 3).start()
        multiply([(0, 2)])
        meanwhile[1]()
        for h in (0, 1):
            for d in (0, 1):
                send2(h, d, 0).wait_recv()
            send2(h, 0, 4).start()
        multiply([(-1, 0), (1, 0)])
        for h in (0, 1):
            for slot in (1, 2):
                for d in (0, 1):
                    send2(h, d, slot).wait_recv()
            send2(h, 0, 5).start()
            send2(h, 1, 4).start()
        multiply([(-1, 1), (1, 3)])
        multiply([(-1, 3), (1, 1)])
        for h in (0, 1):
            for d in (0, 1):
                send2(h, d, 3).wait_recv()
            send2(h, 1, 5).start()
        multiply([(-1, 2), (1, 2)])
        meanwhile[2]()
        for slot in (4, 5):
            for h in (0, 1):
                for d in (0, 1):
                    send2(h, d, slot).wait_recv()
            multiply([(2, GATHER_PASS[0][slot - 4]), (2, GATHER_PASS[1][slot - 4])])
        for h in (0, 1):
            for d in (0, 1):
                for slot in range(2):
                    send1(h, d, slot).wait_send()
                for slot in range(6):
                    send2(h, d, slot).wait_send()

    def exchange(e, stage, i):
        return pltpu.make_async_remote_copy(
            ex_s.at[e, stage],
            ex_r.at[e, stage, i - 1],
            ex_send.at[e, stage, i - 1],
            ex_recv.at[e, stage, i - 1],
            device_id={"rows": line(i)[stage if e < 5 else 1 - stage]},
            device_id_type=MESH,
        )

    def exchange_start(e, stage):
        for i in range(1, SIDE):
            exchange(e, stage, i).start()

    def exchange_sum(e, stage):
        total = ex_s[e, stage]
        for i in range(1, SIDE):
            exchange(e, stage, i).wait()
            total = total + ex_r[e, stage, i - 1]
        return total

    def exchange_turn(e):
        ex_s[e, 1] = exchange_sum(e, 0)
        exchange_start(e, 1)

    def total(values):
        return jnp.sum(values, axis=0, keepdims=True)

    def low(values):
        return values.astype(BF16).astype(F32)

    def nothing():
        pass

    def keep(store, everything):
        def done(h, sums):
            for j in (0, 1):
                rows = pl.ds(h * half + j * quarter, quarter)
                store[rows] = sums[j]
                at = pl.multiple_of(row * block + h * half + j * quarter, quarter)
                everything[pl.ds(at, quarter)] = sums[j].astype(BF16)
            gather_start(everything, h)

        return done

    bound = jnp.max(jnp.abs(regrouped[...].astype(F32)), axis=0, keepdims=True) * depth
    for e in (4, 5):
        ex_s[e, 0] = jnp.broadcast_to(jnp.maximum(bound, 1e-30), ex_s.shape[2:])
        exchange_start(e, 0)

    def bounds_turn():
        for e in (4, 5):
            exchange_turn(e)

    def bounds_end():
        for e in (4, 5):
            for i in range(1, SIDE):
                exchange(e, 1, i).wait()

    def sender_bound(stage, h, d, summed, here):
        e = 4 + h
        if here:
            limit = ex_s[e, stage - 1, pl.ds(0, 1)]
            return limit + ex_r[e, stage - 1, 2 * d, pl.ds(0, 1)] if summed else limit
        limit = ex_r[e, stage - 1, 2 * d, pl.ds(0, 1)]
        return limit + ex_r[e, stage - 1, 1, pl.ds(0, 1)] if summed else limit

    def power_code(values, stage, h, d, summed):
        q = values * (SPAN / sender_bound(stage, h, d, summed, True))
        q2 = q * q
        return ((q * jnp.abs(q)) * q2 * (q2 * q2)).astype(BF16)

    def power_decode(values, stage, h, d, summed):
        y = values.astype(F32)
        root = jnp.exp(jnp.log(jnp.maximum(jnp.abs(y), 2.0**-126)) * 0.125)
        return jnp.where(y < 0, -root, root) * (sender_bound(stage, h, d, summed, False) / SPAN)

    def plain_code(values, stage, h, d, summed):
        return values.astype(BF16)

    def plain_decode(values, stage, h, d, summed):
        return values.astype(F32)

    drain = reduce_scatter(
        regrouped, power_code, power_decode, bounds_turn, bounds_end, keep(target, dir_all)
    )
    gather_and_multiply(dir_all, fit_one, (nothing, drain, nothing))

    fit_low[...] = fit_one[...].astype(BF16)

    ex_s[0, 0] = jnp.zeros_like(ex_s[0, 0])
    ex_s[0, 0, pl.ds(0, 1)] = total(target[...] * target[...])
    ex_s[0, 0, pl.ds(1, 1)] = total(fit_one[...] * fit_low[...].astype(F32)) + ridge * total(
        low(target[...]) * target[...]
    )
    exchange_start(0, 0)

    drain = reduce_scatter(
        fit_low, plain_code, plain_decode,
        functools.partial(exchange_turn, 0), nothing, keep(image, image_all),
    )
    sums = exchange_sum(0, 1)
    first_norms = sums[0:1]
    alpha_one = first_norms / sums[1:2]

    def residual_one():
        return target[...] - alpha_one * (image[...] + ridge * target[...])

    ex_s[1, 0] = jnp.zeros_like(ex_s[1, 0])
    ex_s[1, 0, pl.ds(0, 1)] = total(residual_one() * residual_one())
    exchange_start(1, 0)

    def middle():
        exchange_turn(1)
        drain()

    gather_and_multiply(image_all, fit_two, (nothing, middle, nothing))
    norm_one = exchange_sum(1, 1)[0:1]
    beta = norm_one / first_norms
    fit_two[...] = (1 + beta - alpha_one * ridge) * fit_one[...] - alpha_one * fit_two[...]
    fit_low[...] = fit_two[...].astype(BF16)

    ex_s[2, 0] = jnp.zeros_like(ex_s[2, 0])
    residual = residual_one()
    direction = residual + beta * target[...]
    w_ref[...] = alpha_one * target[...]
    image[...] = residual
    target[...] = direction
    ex_s[2, 0, pl.ds(0, 1)] = total(fit_two[...] * fit_low[...].astype(F32)) + ridge * total(
        low(target[...]) * target[...]
    )
    exchange_start(2, 0)

    def second_weights():
        alpha_two = norm_one / exchange_sum(2, 1)[0:1]
        ex_s[3, 1, pl.ds(0, 1)] = alpha_two
        w_ref[...] = w_ref[...] + alpha_two * target[...]

    def residual_two(h, sums):
        alpha_two = ex_s[3, 1, pl.ds(0, 1)]
        squares = None
        for j in (0, 1):
            rows = pl.ds(h * half + j * quarter, quarter)
            left = image[rows] - alpha_two * (sums[j] + ridge * target[rows])
            square = total(left * left)
            squares = square if squares is None else squares + square
        ex_s[3, 0, pl.ds(h, 1)] = squares

    ex_s[3, 0] = jnp.zeros_like(ex_s[3, 0])
    drain = reduce_scatter(
        fit_low, plain_code, plain_decode,
        functools.partial(exchange_turn, 2), second_weights, residual_two,
    )
    exchange_start(3, 0)
    exchange_turn(3)
    drain()
    squares = exchange_sum(3, 1)
    rn_ref[...] = jnp.sqrt((squares[0:1] + squares[1:2]) / first_norms)


def per_device(cols_size, margins, subset_masks, ridge_param):
    depth, examples = subset_masks.shape
    evals = margins.shape[1] // cols_size
    block = examples // (SIDE * SIDE)
    half, quarter = block // 2, block // 4
    vmem = pl.BlockSpec(memory_space=pltpu.VMEM)
    first = (2, 2, 6, half, evals)
    second = (2, 2, 3, quarter, evals)
    weights, norms = pl.pallas_call(
        functools.partial(fit, cols_size),
        out_shape=(
            jax.ShapeDtypeStruct((block, evals), F32),
            jax.ShapeDtypeStruct((1, evals), F32),
        ),
        in_specs=[
            pl.BlockSpec(memory_space=pltpu.SMEM),
            pl.BlockSpec(memory_space=pl.ANY),
            pl.BlockSpec(memory_space=pl.ANY),
        ],
        out_specs=(vmem, vmem),
        scratch_shapes=[
            pltpu.VMEM((depth, examples), BF16),
            pltpu.VMEM((depth, evals), BF16),
            pltpu.VMEM((examples, evals), BF16),
            pltpu.VMEM((examples, evals), BF16),
            pltpu.VMEM((depth, evals), F32),
            pltpu.VMEM((depth, evals), F32),
            pltpu.VMEM((depth, evals), BF16),
            pltpu.VMEM((2, SIDE, half, evals), F32),
            pltpu.VMEM((block, evals), F32),
            pltpu.VMEM((block, evals), F32),
            pltpu.VMEM(first, BF16),
            pltpu.VMEM(first, BF16),
            pltpu.VMEM(second, BF16),
            pltpu.VMEM(second, BF16),
            pltpu.VMEM((6, 2, 8, evals), F32),
            pltpu.VMEM((6, 2, SIDE - 1, 8, evals), F32),
            pltpu.VMEM(margins.shape, BF16),
            pltpu.SemaphoreType.DMA((LOADS,)),
            pltpu.SemaphoreType.DMA(()),
            pltpu.SemaphoreType.DMA((max(cols_size - 1, 1),)),
            pltpu.SemaphoreType.DMA((max(cols_size - 1, 1),)),
            pltpu.SemaphoreType.DMA((2, 2, 6)),
            pltpu.SemaphoreType.DMA((2, 2, 6)),
            pltpu.SemaphoreType.DMA((2, 2, 3)),
            pltpu.SemaphoreType.DMA((2, 2, 3)),
            pltpu.SemaphoreType.DMA((2, 2, 2)),
            pltpu.SemaphoreType.DMA((2, 2, 2)),
            pltpu.SemaphoreType.DMA((2, 2, 6)),
            pltpu.SemaphoreType.DMA((2, 2, 6)),
            pltpu.SemaphoreType.DMA((6, 2, SIDE - 1)),
            pltpu.SemaphoreType.DMA((6, 2, SIDE - 1)),
        ],
        compiler_params=pltpu.CompilerParams(
            collective_id=0, has_side_effects=True, vmem_limit_bytes=66_000_000
        ),
    )(ridge_param.reshape(1, 1), margins, subset_masks)
    return weights, norms.reshape(evals)


def solution(mesh):
    in_specs = (P(("rows", "cols"), None), P("rows", None), P())
    out_specs = (P("rows", "cols"), P("cols"))
    return jax.shard_map(
        functools.partial(per_device, mesh.shape["cols"]),
        mesh=mesh, in_specs=in_specs, out_specs=out_specs, check_vma=False,
    )
```

```python
import functools

import jax
import jax.numpy as jnp
from jax import lax
from jax.experimental import pallas as pl
from jax.experimental.pallas import tpu as pltpu
from jax.sharding import PartitionSpec as P

MESH = pl.DeviceIdType.MESH
BF16 = jnp.bfloat16
F32 = jnp.float32
SIDE = 4
LOADS = 8

FIRST_SLOT = ({2: 2, 1: 1, 3: 4, 0: 5}, {2: 0, 1: 3, 3: 4, 0: 5})
SPAN = 2.0**15.75
GATHER_ORDER = ((0, 1, 3, 2), (0, 3, 1, 2))
GATHER_PASS = ((0, 3), (1, 2))


def fit(
    cols_size, ridge_ref, margins_hbm, mask_ref, w_ref, rn_ref,
    design, regrouped, dir_all, image_all, fit_one, fit_two, fit_low, own, target, image,
    s1, r1, s2, r2, ex_s, ex_r, margins, w_kept, last_s, last_r,
    load_sem, margins_sem, w_sem, last_send, last_recv, m_send, m_recv, s1_send, s1_recv, s2_send, s2_recv,
    a1_send, a1_recv, a2_send, a2_recv, ex_send, ex_recv,
):
    row = lax.axis_index("rows")
    col = lax.axis_index("cols")
    x, z = lax.div(row, SIDE), lax.rem(row, SIDE)
    depth, examples = design.shape
    rows_size = SIDE * SIDE
    block = examples // rows_size
    half = block // 2
    quarter = half // 2
    evals = target.shape[1]
    per = depth // cols_size
    ridge = ridge_ref[0, 0]

    def row_of(h, u1, u2):
        return lax.rem(u1 + 8, SIDE) * (4 - 3 * h) + lax.rem(u2 + 8, SIDE) * (1 + 3 * h)

    def c1(h):
        return x * (1 - h) + z * h

    def c2(h):
        return z * (1 - h) + x * h

    def first(h, u1, u2):
        return pl.multiple_of(row_of(h, u1, u2) * block + h * half, half)

    def load(i):
        rows = pl.ds(i * (depth // LOADS), depth // LOADS)
        return pltpu.make_async_copy(mask_ref.at[rows], design.at[rows], load_sem.at[i])

    def line(i):
        return lax.rem(x + i, SIDE) * SIDE + z, x * SIDE + lax.rem(z + i, SIDE)

    margins_load = pltpu.make_async_copy(margins_hbm, margins, margins_sem)
    margins_load.start()
    barrier = pltpu.get_barrier_semaphore()
    for i in range(1, rows_size):
        peer = lax.rem(row + i, rows_size)
        pl.semaphore_signal(barrier, inc=1, device_id={"rows": peer}, device_id_type=MESH)
    for i in range(1, cols_size):
        peer = lax.rem(col + i, cols_size)
        pl.semaphore_signal(barrier, inc=1, device_id={"cols": peer}, device_id_type=MESH)
    margins_load.wait()
    for i in range(LOADS):
        load(i).start()
    pl.semaphore_wait(barrier, rows_size + cols_size - 2)

    def hand_over(i):
        peer = lax.rem(col + i, cols_size)
        return pltpu.make_async_remote_copy(
            margins.at[:, pl.ds(pl.multiple_of(peer * evals, evals), evals)],
            regrouped.at[pl.ds(pl.multiple_of(col * per, per), per)],
            m_send.at[i - 1],
            m_recv.at[i - 1],
            device_id={"cols": peer},
            device_id_type=MESH,
        )

    for i in range(1, cols_size):
        hand_over(i).start()
    regrouped[pl.ds(pl.multiple_of(col * per, per), per)] = margins[
        :, pl.ds(pl.multiple_of(col * evals, evals), evals)
    ]

    step = min(16, depth // LOADS)
    for i in range(LOADS):
        load(i).wait()

        @pl.loop(0, depth // LOADS // step)
        def _(j):
            rows = pl.ds(pl.multiple_of(i * (depth // LOADS) + j * step, step), step)
            design[rows] = design[rows] * 2 - 1

    for i in range(1, cols_size):
        hand_over(i).wait()

    def partial(operand, h, u1, u2):
        return lax.dot_general(
            design[:, pl.ds(first(h, u1, u2), half)],
            operand[...],
            (((0,), (0,)), ((), ())),
            preferred_element_type=F32,
        )

    def reduce_scatter(operand, encode, decode, hooks, done):
        def send1(h, d, slot):
            return pltpu.make_async_remote_copy(
                s1.at[h, d, slot],
                r1.at[h, d, slot],
                s1_send.at[h, d, slot],
                s1_recv.at[h, d, slot],
                device_id={"rows": row_of(h, c1(h) + 1 - 2 * d, c2(h))},
                device_id_type=MESH,
            )

        def send2(h, d, slot):
            return pltpu.make_async_remote_copy(
                s2.at[h, d, slot],
                r2.at[h, d, slot],
                s2_send.at[h, d, slot],
                s2_recv.at[h, d, slot],
                device_id={"rows": row_of(h, c1(h), c2(h) + 1 - 2 * d)},
                device_id_type=MESH,
            )

        def parts(i):
            return lax.rem(i, 2), lax.rem(lax.div(i, 2), 2), lax.div(i, 4)

        def send_block(h, d, slot, far, k, add, source):
            target = c1(h) + 2 * far + (1 - far) * (1 - 2 * d)
            here = partial(operand, h, target, c2(h) + k)

            if add is None:
                s1[h, d, slot] = encode(here, 1, h, d, 0)
            else:

                @pl.when(add == 1)
                def _():
                    send1(h, d, source).wait_recv()
                    there = decode(r1[h, d, source], 1, h, d, 0)
                    s1[h, d, slot] = encode(here + there, 1, h, d, 1)

                @pl.when(add == 0)
                def _():
                    s1[h, d, slot] = encode(here, 1, h, d, 0)

            send1(h, d, slot).start()

        @pl.loop(0, 8)
        def _(i):
            h, d, s = parts(i)
            send_block(h, d, s, 1 - (s - d) * (s - d), 2 - s, None, None)

        def own_blocks(low):
            @pl.loop(0, 4)
            def _(i):
                h, k = lax.rem(i, 2), low + lax.div(i, 2)
                own[h, k] = partial(operand, h, c1(h), c2(h) + k)

        hooks[0]()
        own_blocks(2)
        hooks[1]()

        @pl.loop(0, 8)
        def _(i):
            h, d, s = parts(i)
            add = 1 - (s - d) * (s - d)
            send_block(h, d, 2 + s, 1 - add, d + 2 * (1 - s), add, d)

        own_blocks(0)
        hooks[2]()

        @pl.loop(0, 8)
        def _(i):
            h, d, s = parts(i)
            add = d
            d = d + s - 2 * d * s
            send_block(h, d, 4 + s, s * 0, 3 * (1 - s), add, 3 - d)

        hooks[3]()

        def collect(h, k):
            for d in (0, 1):
                slot = FIRST_SLOT[d][k]
                summed = int((d, slot) in ((0, 2), (0, 5), (1, 3), (1, 4)))
                send1(h, d, slot).wait_recv()
                own[h, k] = own[h, k] + decode(r1[h, d, slot], 1, h, d, summed)

        def part(h, k, j):
            return own[h, k, pl.ds(j * quarter, quarter)]

        for h in (0, 1):
            collect(h, 2)
            for d in (0, 1):
                s2[h, d, 0] = encode(part(h, 2, d), 2, h, d, 0)
                send2(h, d, 0).start()

        for d, k in ((0, 1), (1, 3)):
            for h in (0, 1):
                collect(h, k)
                s2[h, d, 1] = encode(part(h, k, 1 - d), 2, h, d, 0)
                send2(h, d, 1).start()
        for d, k in ((0, 1), (1, 3)):
            for h in (0, 1):
                send2(h, d, 0).wait_recv()
                there = decode(r2[h, d, 0], 2, h, d, 0)
                s2[h, d, 2] = encode(part(h, k, d) + there, 2, h, d, 1)
                send2(h, d, 2).start()
        for h in (0, 1):
            collect(h, 0)
        for h in (0, 1):
            sums = []
            for j in (0, 1):
                send2(h, j, 2).wait_recv()
                send2(h, 1 - j, 1).wait_recv()
                sums.append(
                    part(h, 0, j)
                    + decode(r2[h, j, 2], 2, h, j, 1)
                    + decode(r2[h, 1 - j, 1], 2, h, 1 - j, 0)
                )
            done(h, sums)

        def drain():
            @pl.loop(0, 24)
            def _(i):
                send1(lax.rem(i, 2), lax.rem(lax.div(i, 2), 2), lax.div(i, 4)).wait_send()

            @pl.loop(0, 12)
            def _(i):
                send2(lax.rem(i, 2), lax.rem(lax.div(i, 2), 2), lax.div(i, 4)).wait_send()

        return drain

    def gather_steps(everything):
        def copy(rows, sends, recvs, h, d, slot, peer):
            return pltpu.make_async_remote_copy(
                everything.at[rows],
                everything.at[rows],
                sends.at[h, d, slot],
                recvs.at[h, d, slot],
                device_id={"rows": peer},
                device_id_type=MESH,
            )

        def send1(h, d, slot):
            sign = 1 - 2 * d
            if slot == 0:
                rows = pl.ds(first(h, c1(h), c2(h)), half)
            else:
                start = first(h, c1(h), c2(h) - sign) + d * quarter
                rows = pl.ds(pl.multiple_of(start, quarter), quarter)
            return copy(rows, a1_send, a1_recv, h, d, slot, row_of(h, c1(h), c2(h) + sign))

        def send2(h, d, slot):
            sign = 1 - 2 * d
            if slot < 4:
                rows = pl.ds(first(h, c1(h), c2(h) + GATHER_ORDER[d][slot]), half)
            else:
                rows = pl.ds(first(h, c1(h) - sign, c2(h) + GATHER_PASS[d][slot - 4]), half)
            return copy(rows, a2_send, a2_recv, h, d, slot, row_of(h, c1(h) + sign, c2(h)))

        return send1, send2

    def gather_start(everything, h):
        send1, send2 = gather_steps(everything)
        for d in (0, 1):
            send1(h, d, 0).start()
        if h == 1:
            for half_of in (1, 0):
                for d in (0, 1):
                    send2(half_of, d, 0).start()

    def gather_and_multiply(everything, result, meanwhile):
        send1, send2 = gather_steps(everything)
        tile = depth

        def multiply(places, fresh=False):
            starts = [first(h, c1(h) + u1, c2(h) + u2) for h in (0, 1) for u1, u2 in places]

            @pl.loop(0, depth // tile)
            def _(i):
                rows = pl.ds(pl.multiple_of(i * tile, tile), tile)
                total = None
                for start in starts:
                    term = jnp.dot(
                        design[rows, pl.ds(start, half)],
                        everything[pl.ds(start, half)],
                        preferred_element_type=F32,
                    )
                    total = term if total is None else total + term
                result[rows] = total if fresh else result[rows] + total

        multiply([(0, 0)], fresh=True)
        for h in (0, 1):
            for d in (0, 1):
                send1(h, d, 0).wait_recv()
                send1(h, d, 1).start()
        for h in (0, 1):
            for slot in (1, 2):
                for d in (0, 1):
                    send2(h, d, slot).start()
        meanwhile[0]()
        multiply([(0, 1), (0, 3)])
        for h in (0, 1):
            for d in (0, 1):
                send1(h, d, 1).wait_recv()
            for d in (0, 1):
                send2(h, d, 3).start()
        multiply([(0, 2)])
        meanwhile[1]()
        for h in (0, 1):
            for d in (0, 1):
                send2(h, d, 0).wait_recv()
            send2(h, 0, 4).start()
        multiply([(-1, 0), (1, 0)])
        for h in (0, 1):
            for slot in (1, 2):
                for d in (0, 1):
                    send2(h, d, slot).wait_recv()
            send2(h, 0, 5).start()
            send2(h, 1, 4).start()
        multiply([(-1, 1), (1, 3)])
        multiply([(-1, 3), (1, 1)])
        for h in (0, 1):
            for d in (0, 1):
                send2(h, d, 3).wait_recv()
            send2(h, 1, 5).start()
        multiply([(-1, 2), (1, 2)])
        meanwhile[2]()
        for slot in (4, 5):
            for h in (0, 1):
                for d in (0, 1):
                    send2(h, d, slot).wait_recv()
            multiply([(2, GATHER_PASS[0][slot - 4]), (2, GATHER_PASS[1][slot - 4])])
        for h in (0, 1):
            for d in (0, 1):
                for slot in range(2):
                    send1(h, d, slot).wait_send()
                for slot in range(6):
                    send2(h, d, slot).wait_send()

    def exchange(e, stage, i):
        return pltpu.make_async_remote_copy(
            ex_s.at[e, stage],
            ex_r.at[e, stage, i - 1],
            ex_send.at[e, stage, i - 1],
            ex_recv.at[e, stage, i - 1],
            device_id={"rows": line(i)[stage if e < 5 else 1 - stage]},
            device_id_type=MESH,
        )

    def exchange_start(e, stage):
        for i in range(1, SIDE):
            exchange(e, stage, i).start()

    def exchange_sum(e, stage):
        total = ex_s[e, stage]
        for i in range(1, SIDE):
            exchange(e, stage, i).wait()
            total = total + ex_r[e, stage, i - 1]
        return total

    def exchange_turn(e):
        ex_s[e, 1] = exchange_sum(e, 0)
        exchange_start(e, 1)

    def total(values):
        return jnp.sum(values, axis=0, keepdims=True)

    def low(values):
        return values.astype(BF16).astype(F32)

    def nothing():
        pass

    def keep(store, everything):
        def done(h, sums):
            for j in (0, 1):
                rows = pl.ds(h * half + j * quarter, quarter)
                store[rows] = sums[j]
                at = pl.multiple_of(row * block + h * half + j * quarter, quarter)
                everything[pl.ds(at, quarter)] = sums[j].astype(BF16)
            gather_start(everything, h)

        return done

    bound = jnp.max(jnp.abs(regrouped[...].astype(F32)), axis=0, keepdims=True) * depth
    for e in (4, 5):
        ex_s[e, 0] = jnp.broadcast_to(jnp.maximum(bound, 1e-30), ex_s.shape[2:])
        exchange_start(e, 0)

    def bounds_turn():
        for e in (4, 5):
            exchange_turn(e)

    def bounds_end():
        for e in (4, 5):
            for i in range(1, SIDE):
                exchange(e, 1, i).wait()

    def sender_bound(stage, h, d, summed, here):
        e = 4 + h
        if here:
            limit = ex_s[e, stage - 1, pl.ds(0, 1)]
            return limit + ex_r[e, stage - 1, 2 * d, pl.ds(0, 1)] if summed else limit
        limit = ex_r[e, stage - 1, 2 * d, pl.ds(0, 1)]
        return limit + ex_r[e, stage - 1, 1, pl.ds(0, 1)] if summed else limit

    def power_code(values, stage, h, d, summed):
        q = values * (SPAN / sender_bound(stage, h, d, summed, True))
        q2 = q * q
        return ((q * jnp.abs(q)) * q2 * (q2 * q2)).astype(BF16)

    def power_decode(values, stage, h, d, summed):
        y = values.astype(F32)
        root = jnp.exp(jnp.log(jnp.maximum(jnp.abs(y), 2.0**-126)) * 0.125)
        return jnp.where(y < 0, -root, root) * (sender_bound(stage, h, d, summed, False) / SPAN)

    def plain_code(values, stage, h, d, summed):
        return values.astype(BF16)

    def plain_decode(values, stage, h, d, summed):
        return values.astype(F32)

    drain = reduce_scatter(
        regrouped, power_code, power_decode, (nothing, bounds_turn, nothing, bounds_end),
        keep(target, dir_all),
    )
    gather_and_multiply(dir_all, fit_one, (nothing, drain, nothing))

    fit_low[...] = fit_one[...].astype(BF16)

    def first_sums():
        ex_s[0, 0] = jnp.zeros_like(ex_s[0, 0])
        ex_s[0, 0, pl.ds(0, 1)] = total(target[...] * target[...])
        ex_s[0, 0, pl.ds(1, 1)] = total(fit_one[...] * fit_low[...].astype(F32)) + ridge * total(
            low(target[...]) * target[...]
        )
        exchange_start(0, 0)

    drain = reduce_scatter(
        fit_low, plain_code, plain_decode,
        (first_sums, nothing, functools.partial(exchange_turn, 0), nothing),
        keep(image, image_all),
    )
    sums = exchange_sum(0, 1)
    first_norms = sums[0:1]
    alpha_one = first_norms / sums[1:2]

    def residual_one():
        return target[...] - alpha_one * (image[...] + ridge * target[...])

    ex_s[1, 0] = jnp.zeros_like(ex_s[1, 0])
    ex_s[1, 0, pl.ds(0, 1)] = total(residual_one() * residual_one())
    exchange_start(1, 0)

    def middle():
        exchange_turn(1)
        drain()

    gather_and_multiply(image_all, fit_two, (nothing, middle, nothing))
    norm_one = exchange_sum(1, 1)[0:1]
    beta = norm_one / first_norms
    fit_two[...] = (1 + beta - alpha_one * ridge) * fit_one[...] - alpha_one * fit_two[...]
    fit_low[...] = fit_two[...].astype(BF16)

    def second_sums():
        ex_s[2, 0] = jnp.zeros_like(ex_s[2, 0])
        residual = residual_one()
        direction = residual + beta * target[...]
        w_kept[...] = alpha_one * target[...]
        image[...] = residual
        target[...] = direction
        ex_s[2, 0, pl.ds(0, 1)] = total(fit_two[...] * fit_low[...].astype(F32)) + ridge * total(
            low(target[...]) * target[...]
        )
        exchange_start(2, 0)

    w_store = pltpu.make_async_copy(w_kept, w_ref, w_sem)

    def second_weights():
        alpha_two = norm_one / exchange_sum(2, 1)[0:1]
        ex_s[3, 1, pl.ds(0, 1)] = alpha_two
        w_kept[...] = w_kept[...] + alpha_two * target[...]
        w_store.start()

    def residual_two(h, sums):
        alpha_two = ex_s[3, 1, pl.ds(0, 1)]
        squares = None
        for j in (0, 1):
            rows = pl.ds(h * half + j * quarter, quarter)
            left = image[rows] - alpha_two * (sums[j] + ridge * target[rows])
            square = total(left * left)
            squares = square if squares is None else squares + square
        last_s[...] = squares if h == 0 else last_s[...] + squares

    drain = reduce_scatter(
        fit_low, plain_code, plain_decode,
        (second_sums, nothing, functools.partial(exchange_turn, 2), second_weights),
        residual_two,
    )

    def last(i):
        return pltpu.make_async_remote_copy(
            last_s,
            last_r.at[i - 1],
            last_send.at[i - 1],
            last_recv.at[i - 1],
            device_id={"rows": lax.rem(row + i, rows_size)},
            device_id_type=MESH,
        )

    for i in range(1, rows_size):
        last(i).start()
    drain()
    w_store.wait()
    squares = last_s[...]
    for i in range(1, rows_size):
        last(i).wait()
        squares = squares + last_r[i - 1]
    rn_ref[...] = jnp.sqrt(squares / first_norms)


def per_device(cols_size, margins, subset_masks, ridge_param):
    depth, examples = subset_masks.shape
    evals = margins.shape[1] // cols_size
    block = examples // (SIDE * SIDE)
    half, quarter = block // 2, block // 4
    vmem = pl.BlockSpec(memory_space=pltpu.VMEM)
    first = (2, 2, 6, half, evals)
    second = (2, 2, 3, quarter, evals)
    weights, norms = pl.pallas_call(
        functools.partial(fit, cols_size),
        out_shape=(
            jax.ShapeDtypeStruct((block, evals), F32),
            jax.ShapeDtypeStruct((1, evals), F32),
        ),
        in_specs=[
            pl.BlockSpec(memory_space=pltpu.SMEM),
            pl.BlockSpec(memory_space=pl.ANY),
            pl.BlockSpec(memory_space=pl.ANY),
        ],
        out_specs=(pl.BlockSpec(memory_space=pl.ANY), vmem),
        scratch_shapes=[
            pltpu.VMEM((depth, examples), BF16),
            pltpu.VMEM((depth, evals), BF16),
            pltpu.VMEM((examples, evals), BF16),
            pltpu.VMEM((examples, evals), BF16),
            pltpu.VMEM((depth, evals), F32),
            pltpu.VMEM((depth, evals), F32),
            pltpu.VMEM((depth, evals), BF16),
            pltpu.VMEM((2, SIDE, half, evals), F32),
            pltpu.VMEM((block, evals), F32),
            pltpu.VMEM((block, evals), F32),
            pltpu.VMEM(first, BF16),
            pltpu.VMEM(first, BF16),
            pltpu.VMEM(second, BF16),
            pltpu.VMEM(second, BF16),
            pltpu.VMEM((6, 2, 8, evals), F32),
            pltpu.VMEM((6, 2, SIDE - 1, 8, evals), F32),
            pltpu.VMEM(margins.shape, BF16),
            pltpu.VMEM((block, evals), F32),
            pltpu.VMEM((1, evals), F32),
            pltpu.VMEM((SIDE * SIDE - 1, 1, evals), F32),
            pltpu.SemaphoreType.DMA((LOADS,)),
            pltpu.SemaphoreType.DMA(()),
            pltpu.SemaphoreType.DMA(()),
            pltpu.SemaphoreType.DMA((SIDE * SIDE - 1,)),
            pltpu.SemaphoreType.DMA((SIDE * SIDE - 1,)),
            pltpu.SemaphoreType.DMA((max(cols_size - 1, 1),)),
            pltpu.SemaphoreType.DMA((max(cols_size - 1, 1),)),
            pltpu.SemaphoreType.DMA((2, 2, 6)),
            pltpu.SemaphoreType.DMA((2, 2, 6)),
            pltpu.SemaphoreType.DMA((2, 2, 3)),
            pltpu.SemaphoreType.DMA((2, 2, 3)),
            pltpu.SemaphoreType.DMA((2, 2, 2)),
            pltpu.SemaphoreType.DMA((2, 2, 2)),
            pltpu.SemaphoreType.DMA((2, 2, 6)),
            pltpu.SemaphoreType.DMA((2, 2, 6)),
            pltpu.SemaphoreType.DMA((6, 2, SIDE - 1)),
            pltpu.SemaphoreType.DMA((6, 2, SIDE - 1)),
        ],
        compiler_params=pltpu.CompilerParams(
            collective_id=0, has_side_effects=True, vmem_limit_bytes=66_000_000
        ),
    )(ridge_param.reshape(1, 1), margins, subset_masks)
    return weights, norms.reshape(evals)


def solution(mesh):
    in_specs = (P(("rows", "cols"), None), P("rows", None), P())
    out_specs = (P("rows", "cols"), P("cols"))
    return jax.shard_map(
        functools.partial(per_device, mesh.shape["cols"]),
        mesh=mesh, in_specs=in_specs, out_specs=out_specs, check_vma=False,
    )
```

```python
import functools

import jax
import jax.numpy as jnp
from jax import lax
from jax.experimental import pallas as pl
from jax.experimental.pallas import tpu as pltpu
from jax.sharding import PartitionSpec as P

MESH = pl.DeviceIdType.MESH
BF16 = jnp.bfloat16
F32 = jnp.float32
SIDE = 4
LOADS = 8

FIRST_SLOT = ({2: 2, 1: 1, 3: 4, 0: 5}, {2: 0, 1: 3, 3: 4, 0: 5})
SPAN = 2.0**15.75
GATHER_ORDER = ((0, 1, 3, 2), (0, 3, 1, 2))
GATHER_PASS = ((0, 3), (1, 2))


def fit(
    cols_size, ridge_ref, margins_hbm, mask_ref, w_ref, rn_ref,
    design, regrouped, dir_all, image_all, fit_one, fit_two, fit_low, own, target, image,
    s1, r1, s2, r2, ex_s, ex_r, margins, w_kept, last_s, last_r,
    load_sem, margins_sem, w_sem, last_send, last_recv, m_send, m_recv, s1_send, s1_recv, s2_send, s2_recv,
    a1_send, a1_recv, a2_send, a2_recv, ex_send, ex_recv,
):
    row = lax.axis_index("rows")
    col = lax.axis_index("cols")
    x, z = lax.div(row, SIDE), lax.rem(row, SIDE)
    depth, examples = design.shape
    rows_size = SIDE * SIDE
    block = examples // rows_size
    half = block // 2
    quarter = half // 2
    evals = target.shape[1]
    per = depth // cols_size
    ridge = ridge_ref[0, 0]

    def row_of(h, u1, u2):
        return lax.rem(u1 + 8, SIDE) * (4 - 3 * h) + lax.rem(u2 + 8, SIDE) * (1 + 3 * h)

    def c1(h):
        return x * (1 - h) + z * h

    def c2(h):
        return z * (1 - h) + x * h

    def first(h, u1, u2):
        return pl.multiple_of(row_of(h, u1, u2) * block + h * half, half)

    def load(i):
        rows = pl.ds(i * (depth // LOADS), depth // LOADS)
        return pltpu.make_async_copy(mask_ref.at[rows], design.at[rows], load_sem.at[i])

    def line(i):
        return lax.rem(x + i, SIDE) * SIDE + z, x * SIDE + lax.rem(z + i, SIDE)

    margins_load = pltpu.make_async_copy(margins_hbm, margins, margins_sem)
    margins_load.start()
    barrier = pltpu.get_barrier_semaphore()
    for i in range(1, rows_size):
        peer = lax.rem(row + i, rows_size)
        pl.semaphore_signal(barrier, inc=1, device_id={"rows": peer}, device_id_type=MESH)
    for i in range(1, cols_size):
        peer = lax.rem(col + i, cols_size)
        pl.semaphore_signal(barrier, inc=1, device_id={"cols": peer}, device_id_type=MESH)
    margins_load.wait()
    for i in range(LOADS):
        load(i).start()
    pl.semaphore_wait(barrier, rows_size + cols_size - 2)

    def hand_over(i):
        peer = lax.rem(col + i, cols_size)
        return pltpu.make_async_remote_copy(
            margins.at[:, pl.ds(pl.multiple_of(peer * evals, evals), evals)],
            regrouped.at[pl.ds(pl.multiple_of(col * per, per), per)],
            m_send.at[i - 1],
            m_recv.at[i - 1],
            device_id={"cols": peer},
            device_id_type=MESH,
        )

    for i in sorted(range(1, cols_size), key=lambda i: abs(i - cols_size // 2)):
        hand_over(i).start()
    regrouped[pl.ds(pl.multiple_of(col * per, per), per)] = margins[
        :, pl.ds(pl.multiple_of(col * evals, evals), evals)
    ]

    step = min(16, depth // LOADS)
    for i in range(LOADS):
        load(i).wait()

        @pl.loop(0, depth // LOADS // step)
        def _(j):
            rows = pl.ds(pl.multiple_of(i * (depth // LOADS) + j * step, step), step)
            design[rows] = design[rows] * 2 - 1

    for i in range(1, cols_size):
        hand_over(i).wait()

    def partial(operand, h, u1, u2):
        return lax.dot_general(
            design[:, pl.ds(first(h, u1, u2), half)],
            operand[...],
            (((0,), (0,)), ((), ())),
            preferred_element_type=F32,
        )

    def reduce_scatter(operand, encode, decode, hooks, done):
        def send1(h, d, slot):
            return pltpu.make_async_remote_copy(
                s1.at[h, d, slot],
                r1.at[h, d, slot],
                s1_send.at[h, d, slot],
                s1_recv.at[h, d, slot],
                device_id={"rows": row_of(h, c1(h) + 1 - 2 * d, c2(h))},
                device_id_type=MESH,
            )

        def send2(h, d, slot):
            return pltpu.make_async_remote_copy(
                s2.at[h, d, slot],
                r2.at[h, d, slot],
                s2_send.at[h, d, slot],
                s2_recv.at[h, d, slot],
                device_id={"rows": row_of(h, c1(h), c2(h) + 1 - 2 * d)},
                device_id_type=MESH,
            )

        def parts(i):
            return lax.rem(i, 2), lax.rem(lax.div(i, 2), 2), lax.div(i, 4)

        def send_block(h, d, slot, far, k, add, source):
            target = c1(h) + 2 * far + (1 - far) * (1 - 2 * d)
            here = partial(operand, h, target, c2(h) + k)

            if add is None:
                s1[h, d, slot] = encode(here, 1, h, d, 0)
            else:

                @pl.when(add == 1)
                def _():
                    send1(h, d, source).wait_recv()
                    there = decode(r1[h, d, source], 1, h, d, 0)
                    s1[h, d, slot] = encode(here + there, 1, h, d, 1)

                @pl.when(add == 0)
                def _():
                    s1[h, d, slot] = encode(here, 1, h, d, 0)

            send1(h, d, slot).start()

        @pl.loop(0, 8)
        def _(i):
            h, d, s = parts(i)
            send_block(h, d, s, 1 - (s - d) * (s - d), 2 - s, None, None)

        def collect(h, k):
            for d in (0, 1):
                slot = FIRST_SLOT[d][k]
                summed = int((d, slot) in ((0, 2), (0, 5), (1, 3), (1, 4)))
                send1(h, d, slot).wait_recv()
                own[h, k] = own[h, k] + decode(r1[h, d, slot], 1, h, d, summed)

        def part(h, k, j):
            return own[h, k, pl.ds(j * quarter, quarter)]

        def own_blocks(low):
            @pl.loop(0, 4)
            def _(i):
                h, k = lax.rem(i, 2), low + lax.div(i, 2)
                own[h, k] = partial(operand, h, c1(h), c2(h) + k)

        hooks[0]()
        own_blocks(2)
        hooks[1]()

        @pl.loop(0, 8)
        def _(i):
            h, d, s = parts(i)
            add = 1 - (s - d) * (s - d)
            send_block(h, d, 2 + s, 1 - add, d + 2 * (1 - s), add, d)

        own_blocks(0)
        hooks[2]()
        for h in (0, 1):
            collect(h, 2)
            for d in (0, 1):
                s2[h, d, 0] = encode(part(h, 2, d), 2, h, d, 0)
                send2(h, d, 0).start()


        @pl.loop(0, 8)
        def _(i):
            h, d, s = parts(i)
            add = d
            d = d + s - 2 * d * s
            send_block(h, d, 4 + s, s * 0, 3 * (1 - s), add, 3 - d)

        hooks[3]()

        for d, k in ((0, 1), (1, 3)):
            for h in (0, 1):
                collect(h, k)
                s2[h, d, 1] = encode(part(h, k, 1 - d), 2, h, d, 0)
                send2(h, d, 1).start()
        for d, k in ((0, 1), (1, 3)):
            for h in (0, 1):
                send2(h, d, 0).wait_recv()
                there = decode(r2[h, d, 0], 2, h, d, 0)
                s2[h, d, 2] = encode(part(h, k, d) + there, 2, h, d, 1)
                send2(h, d, 2).start()
        for h in (0, 1):
            collect(h, 0)
        for h in (0, 1):
            sums = []
            for j in (0, 1):
                send2(h, j, 2).wait_recv()
                send2(h, 1 - j, 1).wait_recv()
                sums.append(
                    part(h, 0, j)
                    + decode(r2[h, j, 2], 2, h, j, 1)
                    + decode(r2[h, 1 - j, 1], 2, h, 1 - j, 0)
                )
            done(h, sums)

        def drain():
            @pl.loop(0, 24)
            def _(i):
                send1(lax.rem(i, 2), lax.rem(lax.div(i, 2), 2), lax.div(i, 4)).wait_send()

            @pl.loop(0, 12)
            def _(i):
                send2(lax.rem(i, 2), lax.rem(lax.div(i, 2), 2), lax.div(i, 4)).wait_send()

        return drain

    def gather_steps(everything):
        def copy(rows, sends, recvs, h, d, slot, peer):
            return pltpu.make_async_remote_copy(
                everything.at[rows],
                everything.at[rows],
                sends.at[h, d, slot],
                recvs.at[h, d, slot],
                device_id={"rows": peer},
                device_id_type=MESH,
            )

        def send1(h, d, slot):
            sign = 1 - 2 * d
            if slot == 0:
                rows = pl.ds(first(h, c1(h), c2(h)), half)
            else:
                start = first(h, c1(h), c2(h) - sign) + d * quarter
                rows = pl.ds(pl.multiple_of(start, quarter), quarter)
            return copy(rows, a1_send, a1_recv, h, d, slot, row_of(h, c1(h), c2(h) + sign))

        def send2(h, d, slot):
            sign = 1 - 2 * d
            if slot < 4:
                rows = pl.ds(first(h, c1(h), c2(h) + GATHER_ORDER[d][slot]), half)
            else:
                rows = pl.ds(first(h, c1(h) - sign, c2(h) + GATHER_PASS[d][slot - 4]), half)
            return copy(rows, a2_send, a2_recv, h, d, slot, row_of(h, c1(h) + sign, c2(h)))

        return send1, send2

    def gather_start(everything, h):
        send1, send2 = gather_steps(everything)
        for d in (0, 1):
            send1(h, d, 0).start()
        if h == 1:
            for half_of in (1, 0):
                for d in (0, 1):
                    send2(half_of, d, 0).start()

    def gather_and_multiply(everything, result, meanwhile):
        send1, send2 = gather_steps(everything)
        tile = depth

        def multiply(places, fresh=False):
            starts = [first(h, c1(h) + u1, c2(h) + u2) for h in (0, 1) for u1, u2 in places]

            @pl.loop(0, depth // tile)
            def _(i):
                rows = pl.ds(pl.multiple_of(i * tile, tile), tile)
                total = None
                for start in starts:
                    term = jnp.dot(
                        design[rows, pl.ds(start, half)],
                        everything[pl.ds(start, half)],
                        preferred_element_type=F32,
                    )
                    total = term if total is None else total + term
                result[rows] = total if fresh else result[rows] + total

        multiply([(0, 0)], fresh=True)
        for h in (0, 1):
            for d in (0, 1):
                send1(h, d, 0).wait_recv()
                send1(h, d, 1).start()
        for h in (0, 1):
            for slot in (1, 2):
                for d in (0, 1):
                    send2(h, d, slot).start()
        meanwhile[0]()
        multiply([(0, 1), (0, 3)])
        for h in (0, 1):
            for d in (0, 1):
                send1(h, d, 1).wait_recv()
            for d in (0, 1):
                send2(h, d, 3).start()
        multiply([(0, 2)])
        meanwhile[1]()
        for h in (0, 1):
            for d in (0, 1):
                send2(h, d, 0).wait_recv()
            send2(h, 0, 4).start()
        multiply([(-1, 0), (1, 0)])
        for h in (0, 1):
            for slot in (1, 2):
                for d in (0, 1):
                    send2(h, d, slot).wait_recv()
            send2(h, 0, 5).start()
            send2(h, 1, 4).start()
        multiply([(-1, 1), (1, 3)])
        multiply([(-1, 3), (1, 1)])
        for h in (0, 1):
            for d in (0, 1):
                send2(h, d, 3).wait_recv()
            send2(h, 1, 5).start()
        multiply([(-1, 2), (1, 2)])
        meanwhile[2]()
        for slot in (4, 5):
            for h in (0, 1):
                for d in (0, 1):
                    send2(h, d, slot).wait_recv()
            multiply([(2, GATHER_PASS[0][slot - 4]), (2, GATHER_PASS[1][slot - 4])])
        for h in (0, 1):
            for d in (0, 1):
                for slot in range(2):
                    send1(h, d, slot).wait_send()
                for slot in range(6):
                    send2(h, d, slot).wait_send()

    def exchange(e, stage, i):
        return pltpu.make_async_remote_copy(
            ex_s.at[e, stage],
            ex_r.at[e, stage, i - 1],
            ex_send.at[e, stage, i - 1],
            ex_recv.at[e, stage, i - 1],
            device_id={"rows": line(i)[stage if e < 5 else 1 - stage]},
            device_id_type=MESH,
        )

    def exchange_start(e, stage):
        for i in range(1, SIDE):
            exchange(e, stage, i).start()

    def exchange_sum(e, stage):
        total = ex_s[e, stage]
        for i in range(1, SIDE):
            exchange(e, stage, i).wait()
            total = total + ex_r[e, stage, i - 1]
        return total

    def exchange_turn(e):
        ex_s[e, 1] = exchange_sum(e, 0)
        exchange_start(e, 1)

    def total(values):
        return jnp.sum(values, axis=0, keepdims=True)

    def low(values):
        return values.astype(BF16).astype(F32)

    def nothing():
        pass

    def keep(store, everything):
        def done(h, sums):
            for j in (0, 1):
                rows = pl.ds(h * half + j * quarter, quarter)
                store[rows] = sums[j]
                at = pl.multiple_of(row * block + h * half + j * quarter, quarter)
                everything[pl.ds(at, quarter)] = sums[j].astype(BF16)
            gather_start(everything, h)

        return done

    bound = jnp.max(jnp.abs(regrouped[...].astype(F32)), axis=0, keepdims=True) * depth
    for e in (4, 5):
        ex_s[e, 0] = jnp.broadcast_to(jnp.maximum(bound, 1e-30), ex_s.shape[2:])
        exchange_start(e, 0)

    def bounds_turn():
        for e in (4, 5):
            exchange_turn(e)

    def bounds_end():
        for e in (4, 5):
            for i in range(1, SIDE):
                exchange(e, 1, i).wait()

    def sender_bound(stage, h, d, summed, here):
        e = 4 + h
        if here:
            limit = ex_s[e, stage - 1, pl.ds(0, 1)]
            return limit + ex_r[e, stage - 1, 2 * d, pl.ds(0, 1)] if summed else limit
        limit = ex_r[e, stage - 1, 2 * d, pl.ds(0, 1)]
        return limit + ex_r[e, stage - 1, 1, pl.ds(0, 1)] if summed else limit

    def power_code(values, stage, h, d, summed):
        q = values * (SPAN / sender_bound(stage, h, d, summed, True))
        q2 = q * q
        return ((q * jnp.abs(q)) * q2 * (q2 * q2)).astype(BF16)

    def power_decode(values, stage, h, d, summed):
        y = values.astype(F32)
        root = jnp.exp(jnp.log(jnp.maximum(jnp.abs(y), 2.0**-126)) * 0.125)
        return jnp.where(y < 0, -root, root) * (sender_bound(stage, h, d, summed, False) / SPAN)

    def plain_code(values, stage, h, d, summed):
        return values.astype(BF16)

    def plain_decode(values, stage, h, d, summed):
        return values.astype(F32)

    drain = reduce_scatter(
        regrouped, power_code, power_decode, (nothing, bounds_turn, bounds_end, nothing),
        keep(target, dir_all),
    )
    gather_and_multiply(dir_all, fit_one, (drain, nothing, nothing))

    fit_low[...] = fit_one[...].astype(BF16)

    def first_sums():
        ex_s[0, 0] = jnp.zeros_like(ex_s[0, 0])
        ex_s[0, 0, pl.ds(0, 1)] = total(target[...] * target[...])
        ex_s[0, 0, pl.ds(1, 1)] = total(fit_one[...] * fit_low[...].astype(F32)) + ridge * total(
            low(target[...]) * target[...]
        )
        exchange_start(0, 0)

    drain = reduce_scatter(
        fit_low, plain_code, plain_decode,
        (first_sums, nothing, functools.partial(exchange_turn, 0), nothing),
        keep(image, image_all),
    )
    sums = exchange_sum(0, 1)
    first_norms = sums[0:1]
    alpha_one = first_norms / sums[1:2]

    def residual_one():
        return target[...] - alpha_one * (image[...] + ridge * target[...])

    ex_s[1, 0] = jnp.zeros_like(ex_s[1, 0])
    ex_s[1, 0, pl.ds(0, 1)] = total(residual_one() * residual_one())
    exchange_start(1, 0)

    gather_and_multiply(image_all, fit_two, (drain, functools.partial(exchange_turn, 1), nothing))
    norm_one = exchange_sum(1, 1)[0:1]
    beta = norm_one / first_norms
    fit_two[...] = (1 + beta - alpha_one * ridge) * fit_one[...] - alpha_one * fit_two[...]
    fit_low[...] = fit_two[...].astype(BF16)

    def second_sums():
        ex_s[2, 0] = jnp.zeros_like(ex_s[2, 0])
        residual = residual_one()
        direction = residual + beta * target[...]
        w_kept[...] = alpha_one * target[...]
        image[...] = residual
        target[...] = direction
        ex_s[2, 0, pl.ds(0, 1)] = total(fit_two[...] * fit_low[...].astype(F32)) + ridge * total(
            low(target[...]) * target[...]
        )
        exchange_start(2, 0)

    w_store = pltpu.make_async_copy(w_kept, w_ref, w_sem)

    def second_weights():
        alpha_two = norm_one / exchange_sum(2, 1)[0:1]
        ex_s[3, 1, pl.ds(0, 1)] = alpha_two
        w_kept[...] = w_kept[...] + alpha_two * target[...]
        w_store.start()

    def residual_two(h, sums):
        alpha_two = ex_s[3, 1, pl.ds(0, 1)]
        squares = None
        for j in (0, 1):
            rows = pl.ds(h * half + j * quarter, quarter)
            left = image[rows] - alpha_two * (sums[j] + ridge * target[rows])
            square = total(left * left)
            squares = square if squares is None else squares + square
        last_s[...] = squares if h == 0 else last_s[...] + squares

    drain = reduce_scatter(
        fit_low, plain_code, plain_decode,
        (second_sums, nothing, functools.partial(exchange_turn, 2), second_weights),
        residual_two,
    )

    def last(i):
        return pltpu.make_async_remote_copy(
            last_s,
            last_r.at[i - 1],
            last_send.at[i - 1],
            last_recv.at[i - 1],
            device_id={"rows": lax.rem(row + i, rows_size)},
            device_id_type=MESH,
        )

    for i in range(1, rows_size):
        last(i).start()
    drain()
    w_store.wait()
    squares = last_s[...]
    for i in range(1, rows_size):
        last(i).wait()
        squares = squares + last_r[i - 1]
    rn_ref[...] = jnp.sqrt(squares / first_norms)


def per_device(cols_size, margins, subset_masks, ridge_param):
    depth, examples = subset_masks.shape
    evals = margins.shape[1] // cols_size
    block = examples // (SIDE * SIDE)
    half, quarter = block // 2, block // 4
    vmem = pl.BlockSpec(memory_space=pltpu.VMEM)
    first = (2, 2, 6, half, evals)
    second = (2, 2, 3, quarter, evals)
    weights, norms = pl.pallas_call(
        functools.partial(fit, cols_size),
        out_shape=(
            jax.ShapeDtypeStruct((block, evals), F32),
            jax.ShapeDtypeStruct((1, evals), F32),
        ),
        in_specs=[
            pl.BlockSpec(memory_space=pltpu.SMEM),
            pl.BlockSpec(memory_space=pl.ANY),
            pl.BlockSpec(memory_space=pl.ANY),
        ],
        out_specs=(pl.BlockSpec(memory_space=pl.ANY), vmem),
        scratch_shapes=[
            pltpu.VMEM((depth, examples), BF16),
            pltpu.VMEM((depth, evals), BF16),
            pltpu.VMEM((examples, evals), BF16),
            pltpu.VMEM((examples, evals), BF16),
            pltpu.VMEM((depth, evals), F32),
            pltpu.VMEM((depth, evals), F32),
            pltpu.VMEM((depth, evals), BF16),
            pltpu.VMEM((2, SIDE, half, evals), F32),
            pltpu.VMEM((block, evals), F32),
            pltpu.VMEM((block, evals), F32),
            pltpu.VMEM(first, BF16),
            pltpu.VMEM(first, BF16),
            pltpu.VMEM(second, BF16),
            pltpu.VMEM(second, BF16),
            pltpu.VMEM((6, 2, 8, evals), F32),
            pltpu.VMEM((6, 2, SIDE - 1, 8, evals), F32),
            pltpu.VMEM(margins.shape, BF16),
            pltpu.VMEM((block, evals), F32),
            pltpu.VMEM((1, evals), F32),
            pltpu.VMEM((SIDE * SIDE - 1, 1, evals), F32),
            pltpu.SemaphoreType.DMA((LOADS,)),
            pltpu.SemaphoreType.DMA(()),
            pltpu.SemaphoreType.DMA(()),
            pltpu.SemaphoreType.DMA((SIDE * SIDE - 1,)),
            pltpu.SemaphoreType.DMA((SIDE * SIDE - 1,)),
            pltpu.SemaphoreType.DMA((max(cols_size - 1, 1),)),
            pltpu.SemaphoreType.DMA((max(cols_size - 1, 1),)),
            pltpu.SemaphoreType.DMA((2, 2, 6)),
            pltpu.SemaphoreType.DMA((2, 2, 6)),
            pltpu.SemaphoreType.DMA((2, 2, 3)),
            pltpu.SemaphoreType.DMA((2, 2, 3)),
            pltpu.SemaphoreType.DMA((2, 2, 2)),
            pltpu.SemaphoreType.DMA((2, 2, 2)),
            pltpu.SemaphoreType.DMA((2, 2, 6)),
            pltpu.SemaphoreType.DMA((2, 2, 6)),
            pltpu.SemaphoreType.DMA((6, 2, SIDE - 1)),
            pltpu.SemaphoreType.DMA((6, 2, SIDE - 1)),
        ],
        compiler_params=pltpu.CompilerParams(
            collective_id=0, has_side_effects=True, vmem_limit_bytes=66_000_000
        ),
    )(ridge_param.reshape(1, 1), margins, subset_masks)
    return weights, norms.reshape(evals)


def solution(mesh):
    in_specs = (P(("rows", "cols"), None), P("rows", None), P())
    out_specs = (P("rows", "cols"), P("cols"))
    return jax.shard_map(
        functools.partial(per_device, mesh.shape["cols"]),
        mesh=mesh, in_specs=in_specs, out_specs=out_specs, check_vma=False,
    )
```

```python
import functools

import jax
import jax.numpy as jnp
from jax import lax
from jax.experimental import pallas as pl
from jax.experimental.pallas import tpu as pltpu
from jax.sharding import PartitionSpec as P

MESH = pl.DeviceIdType.MESH
BF16 = jnp.bfloat16
F32 = jnp.float32
SIDE = 4
LOADS = 8

FIRST_SLOT = ({2: 2, 1: 1, 3: 4, 0: 5}, {2: 0, 1: 3, 3: 4, 0: 5})
SPAN = 2.0**15.75
GATHER_ORDER = ((0, 1, 3, 2), (0, 3, 1, 2))
GATHER_PASS = ((0, 3), (1, 2))


def fit(
    cols_size, ridge_ref, margins_hbm, mask_ref, w_ref, rn_ref,
    design, regrouped, dir_all, image_all, fit_one, fit_two, fit_low, own, target, image,
    s1, r1, s2, r2, ex_s, ex_r, margins, w_kept, last_s, last_r,
    load_sem, margins_sem, w_sem, last_send, last_recv, m_send, m_recv, s1_send, s1_recv, s2_send, s2_recv,
    a1_send, a1_recv, a2_send, a2_recv, ex_send, ex_recv,
):
    row = lax.axis_index("rows")
    col = lax.axis_index("cols")
    x, z = lax.div(row, SIDE), lax.rem(row, SIDE)
    depth, examples = design.shape
    rows_size = SIDE * SIDE
    block = examples // rows_size
    half = block // 2
    quarter = half // 2
    evals = target.shape[1]
    per = depth // cols_size
    ridge = ridge_ref[0, 0]

    def row_of(h, u1, u2):
        return lax.rem(u1 + 8, SIDE) * (4 - 3 * h) + lax.rem(u2 + 8, SIDE) * (1 + 3 * h)

    def c1(h):
        return x * (1 - h) + z * h

    def c2(h):
        return z * (1 - h) + x * h

    def first(h, u1, u2):
        return pl.multiple_of(row_of(h, u1, u2) * block + h * half, half)

    def load(i):
        rows = pl.ds(i * (depth // LOADS), depth // LOADS)
        return pltpu.make_async_copy(mask_ref.at[rows], design.at[rows], load_sem.at[i])

    def line(i):
        return lax.rem(x + i, SIDE) * SIDE + z, x * SIDE + lax.rem(z + i, SIDE)

    margins_load = pltpu.make_async_copy(margins_hbm, margins, margins_sem)
    margins_load.start()
    barrier = pltpu.get_barrier_semaphore()
    for i in range(1, rows_size):
        peer = lax.rem(row + i, rows_size)
        pl.semaphore_signal(barrier, inc=1, device_id={"rows": peer}, device_id_type=MESH)
    for i in range(1, cols_size):
        peer = lax.rem(col + i, cols_size)
        pl.semaphore_signal(barrier, inc=1, device_id={"cols": peer}, device_id_type=MESH)
    margins_load.wait()
    for i in range(LOADS):
        load(i).start()
    pl.semaphore_wait(barrier, rows_size + cols_size - 2)

    def hand_over(i):
        peer = lax.rem(col + i, cols_size)
        return pltpu.make_async_remote_copy(
            margins.at[:, pl.ds(pl.multiple_of(peer * evals, evals), evals)],
            regrouped.at[pl.ds(pl.multiple_of(col * per, per), per)],
            m_send.at[i - 1],
            m_recv.at[i - 1],
            device_id={"cols": peer},
            device_id_type=MESH,
        )

    for i in sorted(range(1, cols_size), key=lambda i: abs(i - cols_size // 2)):
        hand_over(i).start()
    regrouped[pl.ds(pl.multiple_of(col * per, per), per)] = margins[
        :, pl.ds(pl.multiple_of(col * evals, evals), evals)
    ]

    step = min(16, depth // LOADS)
    for i in range(LOADS):
        load(i).wait()

        @pl.loop(0, depth // LOADS // step)
        def _(j):
            rows = pl.ds(pl.multiple_of(i * (depth // LOADS) + j * step, step), step)
            design[rows] = design[rows] * 2 - 1

    for i in range(1, cols_size):
        hand_over(i).wait()

    def partial(operand, h, u1, u2):
        return lax.dot_general(
            design[:, pl.ds(first(h, u1, u2), half)],
            operand[...],
            (((0,), (0,)), ((), ())),
            preferred_element_type=F32,
        )

    def reduce_scatter(operand, encode, decode, hooks, done):
        def send1(h, d, slot):
            return pltpu.make_async_remote_copy(
                s1.at[h, d, slot],
                r1.at[h, d, slot],
                s1_send.at[h, d, slot],
                s1_recv.at[h, d, slot],
                device_id={"rows": row_of(h, c1(h) + 1 - 2 * d, c2(h))},
                device_id_type=MESH,
            )

        def send2(h, d, slot):
            return pltpu.make_async_remote_copy(
                s2.at[h, d, slot],
                r2.at[h, d, slot],
                s2_send.at[h, d, slot],
                s2_recv.at[h, d, slot],
                device_id={"rows": row_of(h, c1(h), c2(h) + 1 - 2 * d)},
                device_id_type=MESH,
            )

        def parts(i):
            return lax.rem(i, 2), lax.rem(lax.div(i, 2), 2), lax.div(i, 4)

        def send_block(h, d, slot, far, k, add, source):
            target = c1(h) + 2 * far + (1 - far) * (1 - 2 * d)
            here = partial(operand, h, target, c2(h) + k)

            if add is None:
                s1[h, d, slot] = encode(here, 1, h, d, 0)
            else:

                @pl.when(add == 1)
                def _():
                    send1(h, d, source).wait_recv()
                    there = decode(r1[h, d, source], 1, h, d, 0)
                    s1[h, d, slot] = encode(here + there, 1, h, d, 1)

                @pl.when(add == 0)
                def _():
                    s1[h, d, slot] = encode(here, 1, h, d, 0)

            send1(h, d, slot).start()

        @pl.loop(0, 8)
        def _(i):
            h, d, s = parts(i)
            send_block(h, d, s, 1 - (s - d) * (s - d), 2 - s, None, None)

        def collect(h, k):
            for d in (0, 1):
                slot = FIRST_SLOT[d][k]
                summed = int((d, slot) in ((0, 2), (0, 5), (1, 3), (1, 4)))
                send1(h, d, slot).wait_recv()
                own[h, k] = own[h, k] + decode(r1[h, d, slot], 1, h, d, summed)

        def part(h, k, j):
            return own[h, k, pl.ds(j * quarter, quarter)]

        def own_blocks(low):
            @pl.loop(0, 4)
            def _(i):
                h, k = lax.rem(i, 2), low + lax.div(i, 2)
                own[h, k] = partial(operand, h, c1(h), c2(h) + k)

        hooks[0]()
        own_blocks(2)
        hooks[1]()

        @pl.loop(0, 8)
        def _(i):
            h, d, s = parts(i)
            add = 1 - (s - d) * (s - d)
            send_block(h, d, 2 + s, 1 - add, d + 2 * (1 - s), add, d)

        own_blocks(0)
        hooks[2]()
        for h in (0, 1):
            collect(h, 2)
            for d in (0, 1):
                s2[h, d, 0] = encode(part(h, 2, d), 2, h, d, 0)
                send2(h, d, 0).start()


        @pl.loop(0, 8)
        def _(i):
            h, d, s = parts(i)
            add = d
            d = d + s - 2 * d * s
            send_block(h, d, 4 + s, s * 0, 3 * (1 - s), add, 3 - d)

        hooks[3]()

        for d, k in ((0, 1), (1, 3)):
            for h in (0, 1):
                collect(h, k)
                s2[h, d, 1] = encode(part(h, k, 1 - d), 2, h, d, 0)
                send2(h, d, 1).start()
        for d, k in ((0, 1), (1, 3)):
            for h in (0, 1):
                send2(h, d, 0).wait_recv()
                there = decode(r2[h, d, 0], 2, h, d, 0)
                s2[h, d, 2] = encode(part(h, k, d) + there, 2, h, d, 1)
                send2(h, d, 2).start()
        for h in (0, 1):
            collect(h, 0)
        for h in (0, 1):
            sums = []
            for j in (0, 1):
                send2(h, j, 2).wait_recv()
                send2(h, 1 - j, 1).wait_recv()
                sums.append(
                    part(h, 0, j)
                    + decode(r2[h, j, 2], 2, h, j, 1)
                    + decode(r2[h, 1 - j, 1], 2, h, 1 - j, 0)
                )
            done(h, sums)

        def drain():
            @pl.loop(0, 24)
            def _(i):
                send1(lax.rem(i, 2), lax.rem(lax.div(i, 2), 2), lax.div(i, 4)).wait_send()

            @pl.loop(0, 12)
            def _(i):
                send2(lax.rem(i, 2), lax.rem(lax.div(i, 2), 2), lax.div(i, 4)).wait_send()

        return drain

    def gather_steps(everything):
        def copy(rows, sends, recvs, h, d, slot, peer):
            return pltpu.make_async_remote_copy(
                everything.at[rows],
                everything.at[rows],
                sends.at[h, d, slot],
                recvs.at[h, d, slot],
                device_id={"rows": peer},
                device_id_type=MESH,
            )

        def send1(h, d, slot):
            sign = 1 - 2 * d
            if slot == 0:
                rows = pl.ds(first(h, c1(h), c2(h)), half)
            else:
                start = first(h, c1(h), c2(h) - sign) + d * quarter
                rows = pl.ds(pl.multiple_of(start, quarter), quarter)
            return copy(rows, a1_send, a1_recv, h, d, slot, row_of(h, c1(h), c2(h) + sign))

        def send2(h, d, slot):
            sign = 1 - 2 * d
            if slot < 4:
                rows = pl.ds(first(h, c1(h), c2(h) + GATHER_ORDER[d][slot]), half)
            else:
                rows = pl.ds(first(h, c1(h) - sign, c2(h) + GATHER_PASS[d][slot - 4]), half)
            return copy(rows, a2_send, a2_recv, h, d, slot, row_of(h, c1(h) + sign, c2(h)))

        return send1, send2

    def gather_start(everything, h):
        send1, send2 = gather_steps(everything)
        for d in (0, 1):
            send1(h, d, 0).start()
        if h == 1:
            for half_of in (1, 0):
                for d in (0, 1):
                    send2(half_of, d, 0).start()

    def gather_and_multiply(everything, result, meanwhile):
        send1, send2 = gather_steps(everything)
        tile = depth

        def multiply(places, fresh=False):
            starts = [first(h, c1(h) + u1, c2(h) + u2) for h in (0, 1) for u1, u2 in places]

            @pl.loop(0, depth // tile)
            def _(i):
                rows = pl.ds(pl.multiple_of(i * tile, tile), tile)
                total = None
                for start in starts:
                    term = jnp.dot(
                        design[rows, pl.ds(start, half)],
                        everything[pl.ds(start, half)],
                        preferred_element_type=F32,
                    )
                    total = term if total is None else total + term
                result[rows] = total if fresh else result[rows] + total

        multiply([(0, 0)], fresh=True)
        for h in (0, 1):
            for d in (0, 1):
                send1(h, d, 0).wait_recv()
                send1(h, d, 1).start()
        for h in (0, 1):
            for slot in (1, 2):
                for d in (0, 1):
                    send2(h, d, slot).start()
        meanwhile[0]()
        multiply([(0, 1), (0, 3)])
        for h in (0, 1):
            for d in (0, 1):
                send1(h, d, 1).wait_recv()
            for d in (0, 1):
                send2(h, d, 3).start()
        for h in (0, 1):
            for d in (0, 1):
                send2(h, d, 0).wait_recv()
            send2(h, 0, 4).start()
        multiply([(0, 2)])
        meanwhile[1]()
        multiply([(-1, 0), (1, 0)])
        for h in (0, 1):
            for slot in (1, 2):
                for d in (0, 1):
                    send2(h, d, slot).wait_recv()
            send2(h, 0, 5).start()
            send2(h, 1, 4).start()
        multiply([(-1, 1), (1, 3)])
        multiply([(-1, 3), (1, 1)])
        for h in (0, 1):
            for d in (0, 1):
                send2(h, d, 3).wait_recv()
            send2(h, 1, 5).start()
        multiply([(-1, 2), (1, 2)])
        meanwhile[2]()
        for d, slot in ((0, 4), (1, 4), (0, 5), (1, 5)):
            for h in (0, 1):
                send2(h, d, slot).wait_recv()
            multiply([(2, GATHER_PASS[d][slot - 4])])
        for h in (0, 1):
            for d in (0, 1):
                for slot in range(2):
                    send1(h, d, slot).wait_send()
                for slot in range(6):
                    send2(h, d, slot).wait_send()

    def exchange(e, stage, i):
        return pltpu.make_async_remote_copy(
            ex_s.at[e, stage],
            ex_r.at[e, stage, i - 1],
            ex_send.at[e, stage, i - 1],
            ex_recv.at[e, stage, i - 1],
            device_id={"rows": line(i)[stage if e < 5 else 1 - stage]},
            device_id_type=MESH,
        )

    def exchange_start(e, stage):
        for i in range(1, SIDE):
            exchange(e, stage, i).start()

    def exchange_sum(e, stage):
        total = ex_s[e, stage]
        for i in range(1, SIDE):
            exchange(e, stage, i).wait()
            total = total + ex_r[e, stage, i - 1]
        return total

    def exchange_turn(e):
        ex_s[e, 1] = exchange_sum(e, 0)
        exchange_start(e, 1)

    def total(values):
        return jnp.sum(values, axis=0, keepdims=True)

    def low(values):
        return values.astype(BF16).astype(F32)

    def nothing():
        pass

    def keep(store, everything):
        def done(h, sums):
            for j in (0, 1):
                rows = pl.ds(h * half + j * quarter, quarter)
                store[rows] = sums[j]
                at = pl.multiple_of(row * block + h * half + j * quarter, quarter)
                everything[pl.ds(at, quarter)] = sums[j].astype(BF16)
            gather_start(everything, h)

        return done

    bound = jnp.max(jnp.abs(regrouped[...].astype(F32)), axis=0, keepdims=True) * depth
    for e in (4, 5):
        ex_s[e, 0] = jnp.broadcast_to(jnp.maximum(bound, 1e-30), ex_s.shape[2:])
        exchange_start(e, 0)

    def bounds_turn():
        for e in (4, 5):
            exchange_turn(e)

    def bounds_end():
        for e in (4, 5):
            for i in range(1, SIDE):
                exchange(e, 1, i).wait()

    def sender_bound(stage, h, d, summed, here):
        e = 4 + h
        if here:
            limit = ex_s[e, stage - 1, pl.ds(0, 1)]
            return limit + ex_r[e, stage - 1, 2 * d, pl.ds(0, 1)] if summed else limit
        limit = ex_r[e, stage - 1, 2 * d, pl.ds(0, 1)]
        return limit + ex_r[e, stage - 1, 1, pl.ds(0, 1)] if summed else limit

    def power_code(values, stage, h, d, summed):
        q = values * (SPAN / sender_bound(stage, h, d, summed, True))
        q2 = q * q
        return ((q * jnp.abs(q)) * q2 * (q2 * q2)).astype(BF16)

    def power_decode(values, stage, h, d, summed):
        y = values.astype(F32)
        root = jnp.exp(jnp.log(jnp.maximum(jnp.abs(y), 2.0**-126)) * 0.125)
        return jnp.where(y < 0, -root, root) * (sender_bound(stage, h, d, summed, False) / SPAN)

    def plain_code(values, stage, h, d, summed):
        return values.astype(BF16)

    def plain_decode(values, stage, h, d, summed):
        return values.astype(F32)

    drain = reduce_scatter(
        regrouped, power_code, power_decode, (nothing, bounds_turn, bounds_end, nothing),
        keep(target, dir_all),
    )
    gather_and_multiply(dir_all, fit_one, (drain, nothing, nothing))

    fit_low[...] = fit_one[...].astype(BF16)

    def first_sums():
        ex_s[0, 0] = jnp.zeros_like(ex_s[0, 0])
        ex_s[0, 0, pl.ds(0, 1)] = total(target[...] * target[...])
        ex_s[0, 0, pl.ds(1, 1)] = total(fit_one[...] * fit_low[...].astype(F32)) + ridge * total(
            low(target[...]) * target[...]
        )
        exchange_start(0, 0)

    drain = reduce_scatter(
        fit_low, plain_code, plain_decode,
        (first_sums, nothing, functools.partial(exchange_turn, 0), nothing),
        keep(image, image_all),
    )
    sums = exchange_sum(0, 1)
    first_norms = sums[0:1]
    alpha_one = first_norms / sums[1:2]

    def residual_one():
        return target[...] - alpha_one * (image[...] + ridge * target[...])

    ex_s[1, 0] = jnp.zeros_like(ex_s[1, 0])
    ex_s[1, 0, pl.ds(0, 1)] = total(residual_one() * residual_one())
    exchange_start(1, 0)

    gather_and_multiply(image_all, fit_two, (drain, functools.partial(exchange_turn, 1), nothing))
    norm_one = exchange_sum(1, 1)[0:1]
    beta = norm_one / first_norms
    fit_two[...] = (1 + beta - alpha_one * ridge) * fit_one[...] - alpha_one * fit_two[...]
    fit_low[...] = fit_two[...].astype(BF16)

    def second_sums():
        ex_s[2, 0] = jnp.zeros_like(ex_s[2, 0])
        residual = residual_one()
        direction = residual + beta * target[...]
        w_kept[...] = alpha_one * target[...]
        image[...] = residual
        target[...] = direction
        ex_s[2, 0, pl.ds(0, 1)] = total(fit_two[...] * fit_low[...].astype(F32)) + ridge * total(
            low(target[...]) * target[...]
        )
        exchange_start(2, 0)

    w_store = pltpu.make_async_copy(w_kept, w_ref, w_sem)

    def second_weights():
        alpha_two = norm_one / exchange_sum(2, 1)[0:1]
        ex_s[3, 1, pl.ds(0, 1)] = alpha_two
        w_kept[...] = w_kept[...] + alpha_two * target[...]
        w_store.start()

    def residual_two(h, sums):
        alpha_two = ex_s[3, 1, pl.ds(0, 1)]
        squares = None
        for j in (0, 1):
            rows = pl.ds(h * half + j * quarter, quarter)
            left = image[rows] - alpha_two * (sums[j] + ridge * target[rows])
            square = total(left * left)
            squares = square if squares is None else squares + square
        last_s[...] = squares if h == 0 else last_s[...] + squares

    drain = reduce_scatter(
        fit_low, plain_code, plain_decode,
        (second_sums, nothing, functools.partial(exchange_turn, 2), second_weights),
        residual_two,
    )

    def last(i):
        return pltpu.make_async_remote_copy(
            last_s,
            last_r.at[i - 1],
            last_send.at[i - 1],
            last_recv.at[i - 1],
            device_id={"rows": lax.rem(row + i, rows_size)},
            device_id_type=MESH,
        )

    for i in range(1, rows_size):
        last(i).start()
    drain()
    w_store.wait()
    squares = last_s[...]
    for i in range(1, rows_size):
        last(i).wait()
        squares = squares + last_r[i - 1]
    rn_ref[...] = jnp.sqrt(squares / first_norms)


def per_device(cols_size, margins, subset_masks, ridge_param):
    depth, examples = subset_masks.shape
    evals = margins.shape[1] // cols_size
    block = examples // (SIDE * SIDE)
    half, quarter = block // 2, block // 4
    vmem = pl.BlockSpec(memory_space=pltpu.VMEM)
    first = (2, 2, 6, half, evals)
    second = (2, 2, 3, quarter, evals)
    weights, norms = pl.pallas_call(
        functools.partial(fit, cols_size),
        out_shape=(
            jax.ShapeDtypeStruct((block, evals), F32),
            jax.ShapeDtypeStruct((1, evals), F32),
        ),
        in_specs=[
            pl.BlockSpec(memory_space=pltpu.SMEM),
            pl.BlockSpec(memory_space=pl.ANY),
            pl.BlockSpec(memory_space=pl.ANY),
        ],
        out_specs=(pl.BlockSpec(memory_space=pl.ANY), vmem),
        scratch_shapes=[
            pltpu.VMEM((depth, examples), BF16),
            pltpu.VMEM((depth, evals), BF16),
            pltpu.VMEM((examples, evals), BF16),
            pltpu.VMEM((examples, evals), BF16),
            pltpu.VMEM((depth, evals), F32),
            pltpu.VMEM((depth, evals), F32),
            pltpu.VMEM((depth, evals), BF16),
            pltpu.VMEM((2, SIDE, half, evals), F32),
            pltpu.VMEM((block, evals), F32),
            pltpu.VMEM((block, evals), F32),
            pltpu.VMEM(first, BF16),
            pltpu.VMEM(first, BF16),
            pltpu.VMEM(second, BF16),
            pltpu.VMEM(second, BF16),
            pltpu.VMEM((6, 2, 8, evals), F32),
            pltpu.VMEM((6, 2, SIDE - 1, 8, evals), F32),
            pltpu.VMEM(margins.shape, BF16),
            pltpu.VMEM((block, evals), F32),
            pltpu.VMEM((1, evals), F32),
            pltpu.VMEM((SIDE * SIDE - 1, 1, evals), F32),
            pltpu.SemaphoreType.DMA((LOADS,)),
            pltpu.SemaphoreType.DMA(()),
            pltpu.SemaphoreType.DMA(()),
            pltpu.SemaphoreType.DMA((SIDE * SIDE - 1,)),
            pltpu.SemaphoreType.DMA((SIDE * SIDE - 1,)),
            pltpu.SemaphoreType.DMA((max(cols_size - 1, 1),)),
            pltpu.SemaphoreType.DMA((max(cols_size - 1, 1),)),
            pltpu.SemaphoreType.DMA((2, 2, 6)),
            pltpu.SemaphoreType.DMA((2, 2, 6)),
            pltpu.SemaphoreType.DMA((2, 2, 3)),
            pltpu.SemaphoreType.DMA((2, 2, 3)),
            pltpu.SemaphoreType.DMA((2, 2, 2)),
            pltpu.SemaphoreType.DMA((2, 2, 2)),
            pltpu.SemaphoreType.DMA((2, 2, 6)),
            pltpu.SemaphoreType.DMA((2, 2, 6)),
            pltpu.SemaphoreType.DMA((6, 2, SIDE - 1)),
            pltpu.SemaphoreType.DMA((6, 2, SIDE - 1)),
        ],
        compiler_params=pltpu.CompilerParams(
            collective_id=0, has_side_effects=True, vmem_limit_bytes=66_000_000
        ),
    )(ridge_param.reshape(1, 1), margins, subset_masks)
    return weights, norms.reshape(evals)


def solution(mesh):
    in_specs = (P(("rows", "cols"), None), P("rows", None), P())
    out_specs = (P("rows", "cols"), P("cols"))
    return jax.shard_map(
        functools.partial(per_device, mesh.shape["cols"]),
        mesh=mesh, in_specs=in_specs, out_specs=out_specs, check_vma=False,
    )
```
